32 devices in a mesh: dp: 4 (over z), head: 2 (over y), tok: 4 (over x, core).
Axes of the slice: x: 2, y: 2, z: 4, core: 2. Of those that a mesh axis runs over, the one named last changes fastest.
Arguments:
- mamba_input: bfloat16 [8, 64, 2048], P('dp', 'tok', 'head'), may hold values from -6 to 6
- gate_input: bfloat16 [8, 64, 2048], P('dp', 'tok', 'head'), may hold values from -6 to 6
- in_b: bfloat16 [8, 64, 256], P('dp', 'tok', 'head'), may hold values from -0.75 to 0.75
- in_c: bfloat16 [8, 64, 256], P('dp', 'tok', 'head'), may hold values from -0.75 to 0.75
- step_size: bfloat16 [8, 64, 32], P('dp', 'tok', 'head'), may hold values from 0.019897461 to 1
- decay_rate: float32 [32], P('head'), may hold values from 0.01 to 1
- skip_weight: float32 [32], P('head'), may hold values from 0.5 to 1.5
- norm_gain: float32 [2048], P('head'), may hold values from 0.1 to 1.9
- ssm_state: bfloat16 [8, 32, 64, 128], P('dp', 'head', None, 'tok'), may hold values from -6 to 6
- out_weight: bfloat16 [2048, 4096], P(('head', 'tok')), may hold values from -0.125 to 0.125
- queries: bfloat16 [8, 64, 1024], P('dp', 'tok', 'head'), may hold values from -6 to 6
- draft_token_keys: bfloat16 [8, 64, 256], P('dp', 'tok', 'head'), may hold values from -6 to 6
- draft_values: bfloat16 [8, 64, 256], P('dp', 'tok', 'head'), may hold values from -6 to 6
- cached_key_rows: bfloat16 [8, 4096, 256], P('dp', 'tok', 'head'), may hold values from -4 to 4
- cache_values: bfloat16 [8, 4096, 256], P('dp', 'tok', 'head'), may hold values from -6 to 6
- cache_len: int32 [8], P('dp'), may hold values from 2 to 4096
- accepted: int32 [8], P('dp'), may hold values from 0 to 64
Outputs:
- mamba_out: bfloat16 [64, 8, 4096], P(('head', 'tok'), 'dp')
- attn_context: bfloat16 [8, 64, 1024], P('dp', 'tok', 'head')
- committed_state: bfloat16 [8, 32, 64, 128], P('dp', 'head', None, 'tok')
The draws below stay inside these ranges and needn't reach their ends.
Inputs may be any that keep to these rules, and one draw needn't show every extreme that they name: Each sequence's cached positions 0 to cache_len - 1 are valid.
All inputs are finite; a program needn't handle non-finite values.
Results may differ from the reference program's by a relative error of at most 0.018.
Values may be sent and summed in bfloat16 or wider, within the bound.
A program may use at most 64 MiB of HBM per device.

```python
import math
import jax
import jax.numpy as jnp
from jax import lax

D = 4096
STATE = 128
HEAD_DIM = 64
ATT_DIM = 128
HEADS = 32
GROUPS = 2
QHEADS = 8
KVHEADS = 2
DRAFT = 64
CACHE = 4096
BATCH = 8
N_HEAD = 2
N_TOK = 4


def draw_queries(key, part):
    shape = (BATCH, DRAFT, QHEADS * ATT_DIM)
    base = jnp.clip(jax.random.normal(jax.random.fold_in(key, 11), shape), -4.0, 4.0)
    return base.astype(jnp.bfloat16)


def draw_cached_key_rows(key, part):
    shape = (BATCH, CACHE, KVHEADS * ATT_DIM)
    base = jnp.clip(jax.random.normal(jax.random.fold_in(key, 21), shape), -4.0, 4.0)
    return base.astype(jnp.bfloat16)


def with_ends(result, rng, low, top_value):
    shape = result.shape
    place = [jax.random.randint(jax.random.fold_in(rng, axis), (), 0, shape[axis]) for axis in range(len(shape))]
    result = result.at[tuple(place)].set(low)
    longest = shape.index(max(shape))
    place[longest] = (place[longest] + 1) % shape[longest]
    return result.at[tuple(place)].set(top_value)


def level_of(key, extent, shards, least, high):
    factor_of = 1.0
    for dim, parts in shards:
        steps = jax.random.uniform(jax.random.fold_in(jax.random.fold_in(key, 6), dim), (parts,), jnp.float32, least / len(shards), high / len(shards))
        factor_of = factor_of * jnp.repeat(jnp.exp(steps), extent[dim] // parts).reshape((-1,) + (1,) * (len(extent) - 1 - dim))
    return factor_of


def scatter_about(rng, shape, deviation, bound, cuts=(), dtype=jnp.bfloat16):
    values = deviation * jax.random.normal(rng, shape, jnp.float32)
    if cuts:
        values = values * level_of(rng, shape, cuts, -0.22, 0.18)
    return jnp.clip(values, -bound, bound).astype(dtype)


def setup_inputs(seed: int = 0) -> dict:
    key_of = jax.random.split(jax.random.key(seed), 18)
    return {
        "mamba_input": scatter_about(key_of[0], (BATCH, DRAFT, HEADS * HEAD_DIM), 1.0, 6.0, ((0, 4), (1, 4), (2, 2))),
        "gate_input": scatter_about(key_of[1], (BATCH, DRAFT, HEADS * HEAD_DIM), 1.0, 6.0, ((0, 4), (1, 4), (2, 2))),
        "in_b": scatter_about(key_of[2], (BATCH, DRAFT, GROUPS * STATE), 0.125, 0.75, ((0, 4), (1, 4), (2, 2))),
        "in_c": scatter_about(key_of[3], (BATCH, DRAFT, GROUPS * STATE), 0.125, 0.75, ((0, 4), (1, 4), (2, 2))),
        "step_size": jnp.clip(jnp.exp(math.log(1.0) - 3.9171631 * jax.random.uniform(key_of[4], (BATCH, DRAFT, HEADS), jnp.float32) ** level_of(key_of[4], (BATCH, DRAFT, HEADS), ((0, 4), (1, 4), (2, 2)), -0.2, 0.2)), 0.019897461, 1.0).astype(jnp.bfloat16),
        "decay_rate": jnp.clip(jnp.exp(math.log(1.0) - 4.6051702 * jax.random.uniform(key_of[5], (HEADS,), jnp.float32) ** level_of(key_of[5], (HEADS,), ((0, 2),), -0.2, 0.2)), 0.01, 1.0),
        "skip_weight": jnp.clip(0.5 + 1.0 * jax.random.uniform(key_of[6], (HEADS,), jnp.float32) ** level_of(key_of[6], (HEADS,), ((0, 2),), -0.2, 0.2), 0.5, 1.5),
        "norm_gain": jnp.clip(1.0 + 0.18 * jax.random.normal(key_of[7], (HEADS * HEAD_DIM,), jnp.float32), 0.1, 1.9),
        "ssm_state": scatter_about(key_of[8], (BATCH, HEADS, HEAD_DIM, STATE), 1.0, 6.0, ((0, 4), (1, 2), (3, 4))),
        "out_weight": scatter_about(key_of[9], (HEADS * HEAD_DIM, D), (HEADS * HEAD_DIM) ** -0.5, 0.125, ((0, 8),)),
        "queries": draw_queries(jax.random.fold_in(key_of[17], 71), 0),
        "draft_token_keys": scatter_about(key_of[11], (BATCH, DRAFT, KVHEADS * ATT_DIM), 1.0, 6.0, ((0, 4), (1, 4), (2, 2))),
        "draft_values": scatter_about(key_of[12], (BATCH, DRAFT, KVHEADS * ATT_DIM), 1.0, 6.0, ((0, 4), (1, 4), (2, 2))),
        "cached_key_rows": draw_cached_key_rows(jax.random.fold_in(key_of[17], 71), 0),
        "cache_values": scatter_about(key_of[14], (BATCH, CACHE, KVHEADS * ATT_DIM), 1.0, 6.0, ((0, 4), (1, 4), (2, 2))),
        "cache_len": with_ends(jax.random.randint(key_of[15], (BATCH,), 2, CACHE + 1), jax.random.fold_in(key_of[15], 1), 2, CACHE).astype(jnp.int32),
        "accepted": with_ends(jax.random.randint(key_of[16], (BATCH,), 0, DRAFT + 1), jax.random.fold_in(key_of[16], 1), 0, DRAFT).astype(jnp.int32),
    }


PRECISE = lax.Precision.HIGHEST
EPSILON = 1e-05
MASKED = -1e+30

def attend_one(inputs):
    query_matrix, new_keys, new_values, old_keys, old_values, valid_length = inputs
    draft_len = query_matrix.shape[0]
    kv_heads = new_keys.shape[1] // ATT_DIM
    per_kv = query_matrix.shape[1] // ATT_DIM // kv_heads
    cache_size = old_keys.shape[0]
    queries_f = query_matrix.astype(jnp.float32).reshape(draft_len, kv_heads, per_kv, ATT_DIM)
    keys_f = jnp.concatenate([old_keys, new_keys], axis=0).astype(jnp.float32).reshape(cache_size + draft_len, kv_heads, ATT_DIM)
    values_f = jnp.concatenate([old_values, new_values], axis=0).astype(jnp.float32).reshape(cache_size + draft_len, kv_heads, ATT_DIM)
    scores = jnp.einsum('sgqd,kgd->gsqk', queries_f, keys_f, precision=PRECISE) * ATT_DIM ** (-0.5)
    key_pos = jnp.arange(cache_size + draft_len)
    query_pos = jnp.arange(draft_len)
    allowed = jnp.where(key_pos[None, :] < cache_size, key_pos[None, :] < valid_length, key_pos[None, :] - cache_size <= query_pos[:, None])
    allowed = allowed[None, :, None, :]
    scores = jnp.where(allowed, scores, MASKED)
    row_peak = lax.optimization_barrier(jnp.max(scores, axis=-1, keepdims=True))
    probs = jnp.where(allowed, jnp.exp(scores - row_peak), 0.0)
    totals = lax.optimization_barrier(jnp.sum(probs, axis=-1))
    rounded = lax.optimization_barrier(probs.astype(jnp.bfloat16)).astype(jnp.float32)
    numer = jnp.einsum('gsqk,kgd->gsqd', rounded, values_f, precision=PRECISE)
    context = numer / totals[..., None]
    return jnp.transpose(context, (1, 0, 2, 3)).reshape(draft_len, kv_heads * per_kv * ATT_DIM).astype(jnp.bfloat16)

def reference(mamba_input, gate_input, in_b, in_c, step_size, decay_rate, skip_weight, norm_gain, ssm_state, out_weight, queries, draft_token_keys, draft_values, cached_key_rows, cache_values, cache_len, accepted):
    batch, draft_len, feature_width = mamba_input.shape
    head_count = decay_rate.shape[0]
    group_count = in_b.shape[2] // STATE
    per_group = head_count // group_count
    feature_values = mamba_input.astype(jnp.float32).reshape(batch, draft_len, head_count, HEAD_DIM)
    step_sizes = step_size.astype(jnp.float32)
    inflow = jnp.repeat(in_b.astype(jnp.float32).reshape(batch, draft_len, group_count, STATE), per_group, axis=2)
    readout = jnp.repeat(in_c.astype(jnp.float32).reshape(batch, draft_len, group_count, STATE), per_group, axis=2)
    log_decay = -step_sizes * decay_rate[None, None, :]
    running = jnp.cumsum(log_decay, axis=1)
    position = jnp.arange(draft_len)
    causal = (position[:, None] >= position[None, :])[None, :, :, None]
    log_gaps = jnp.where(causal, running[:, :, None, :] - running[:, None, :, :], 0.0)
    decays = jnp.where(causal, jnp.exp(log_gaps), 0.0)
    affinity = jnp.einsum('bshn,brhn->bsrh', readout, inflow, precision=PRECISE)
    mixing = affinity * decays * step_sizes[:, None, :, :]
    within = jnp.einsum('bsrh,brhp->bshp', mixing, feature_values, precision=PRECISE)
    start_state = ssm_state.astype(jnp.float32)
    carried = jnp.einsum('bshn,bhpn->bshp', readout, start_state, precision=PRECISE) * jnp.exp(running)[..., None]
    mixed = within + carried + skip_weight[None, None, :, None] * feature_values
    gated = mixed.reshape(batch, draft_len, feature_width) * jax.nn.silu(gate_input.astype(jnp.float32))
    grouped = gated.reshape(batch, draft_len, group_count, feature_width // group_count)
    mean_sq = lax.optimization_barrier(jnp.mean(grouped * grouped, axis=-1, keepdims=True))
    normed = (grouped * lax.rsqrt(mean_sq + EPSILON)).reshape(batch, draft_len, feature_width) * norm_gain
    normed = normed.astype(jnp.bfloat16)
    blocks = N_HEAD * N_TOK
    block_rows = feature_width // blocks
    pieces = jnp.transpose(normed.reshape(batch * draft_len, blocks, block_rows), (1, 0, 2))
    weight_blocks = out_weight.reshape(blocks, block_rows, out_weight.shape[1])

    def add_block(accum, pair):
        piece, weight = pair
        part_sum = jnp.dot(piece, weight, preferred_element_type=jnp.float32)
        part_sum = lax.optimization_barrier(part_sum.astype(jnp.bfloat16)).astype(jnp.float32)
        return (accum + part_sum, None)
    summed_total, unused = lax.scan(add_block, jnp.zeros((batch * draft_len, out_weight.shape[1]), jnp.float32), (pieces, weight_blocks))
    mamba_out = jnp.transpose(summed_total.reshape(batch, draft_len, out_weight.shape[1]), (1, 0, 2)).astype(jnp.bfloat16)
    alive = (position[None, :] < accepted[:, None])[..., None]
    end_log = lax.optimization_barrier(jnp.sum(jnp.where(alive, log_decay, 0.0), axis=1))
    weights = jnp.where(alive, jnp.exp(jnp.where(alive, end_log[:, None, :] - running, 0.0)) * step_sizes, 0.0)
    committed = jnp.exp(end_log)[..., None, None] * start_state + jnp.einsum('bsh,bshp,bshn->bhpn', weights, feature_values, inflow, precision=PRECISE)
    committed_state = committed.astype(jnp.bfloat16)
    attn_context = lax.map(attend_one, (queries, draft_token_keys, draft_values, cached_key_rows, cache_values, cache_len))
    return (mamba_out, attn_context, committed_state)
```

```python
import functools
import jax
import jax.numpy as jnp
from jax import lax
from jax.experimental import pallas as pl
from jax.experimental.pallas import tpu as pltpu
from jax.sharding import PartitionSpec as P

EPSILON = 1e-05
MASKED = -1e30
FLOOR = -1e29
MESH = pl.DeviceIdType.MESH
F32 = jnp.float32
BF16 = jnp.bfloat16
NT = (((1,), (1,)), ((), ()))


def dot(a, b):
    return jnp.dot(a, b, preferred_element_type=F32)


def iota(shape, dim):
    return lax.broadcasted_iota(jnp.int32, shape, dim)


def kernel(
    dims,
    x_in, z_in, b_in, c_in, dt_in, st_in, q_in, k_in, v_in, w_in,
    dk_in, dv_in, gain_in, rate_in, skip_in, len_in, acc_in,
    out_ref, ctx_ref, com_ref,
    x_l, z_l, b_l, c_l, dt_l, st_l, q_l, k_v, v_v, w_v, x_v, z_v,
    ss_l, cm_s, cm_l, n_s, n_l, stat_l, part, rs_l,
    dk_ref, dv_ref, gain_ref, raw_v, turn_v, pair_l, red,
    rate_ref, skip_ref, len_ref, acc_ref,
    gat_send, gat_recv, send, recv, ss_send, ss_recv,
    rs_send, rs_recv, pair_send, pair_recv, local,
):
    n_head, n_tok, seqs, block, heads, chunks = dims
    group = n_head * n_tok
    tok = lax.axis_index("tok")
    head = lax.axis_index("head")
    me = head * n_tok + tok
    draft = block * n_tok
    width = x_l.shape[2]
    own = heads // n_tok
    size = width // own
    state = st_l.shape[1]
    cols = state // n_tok
    att = k_v.shape[2]
    per_kv = q_l.shape[2] // att
    cache = k_v.shape[1]
    rows = seqs * draft
    each = rows // group
    out_cols = w_v.shape[1]
    span = out_cols // chunks
    half = group // 2
    side = lax.rem(tok, 2)
    line = tok // 2
    lines = n_tok // 2
    slot = head * lines + line

    def place(index, unit):
        return pl.ds(pl.multiple_of(index * unit, unit), unit)

    barrier = pltpu.get_barrier_semaphore()
    for o in range(1, group):
        peer = lax.rem(me + o, group)
        pl.semaphore_signal(
            barrier, inc=1,
            device_id={"head": peer // n_tok, "tok": lax.rem(peer, n_tok)},
            device_id_type=MESH,
        )

    mine = place(tok, block)
    sources = {
        "st": (st_in, raw_v),
        "q": (q_in, q_l.at[:, mine, :]),
        "b": (b_in, b_l.at[:, mine, :]),
        "c": (c_in, c_l.at[:, mine, :]),
        "dt": (dt_in, dt_l.at[:, mine, :]),
        "x": (x_in, x_v),
        "z": (z_in, z_v),
        "k": (k_in, k_v),
        "v": (v_in, v_v),
        "dk": (dk_in, dk_ref),
        "dv": (dv_in, dv_ref),
        "len": (len_in, len_ref),
        "acc": (acc_in, acc_ref),
        "rate": (rate_in, rate_ref),
        "skip": (skip_in, skip_ref),
        "gain": (gain_in, gain_ref),
        "w": (w_in, w_v),
    }
    held = {}
    for i, (name, (src, dst)) in enumerate(sources.items()):
        held[name] = pltpu.make_async_copy(src, dst, local.at[i])
        held[name].start()

    held["st"].wait()
    for s in range(seqs):
        turn_v[s] = jnp.concatenate(
            [raw_v[s, h].astype(F32) for h in range(heads)], axis=1
        ).astype(BF16)
    st_l[:, place(tok, cols), :] = turn_v[:, :, place(tok, width)]
    for name in ("q", "b", "c", "dt", "x", "z"):
        held[name].wait()
    x_l[:, mine, :] = x_v[:, :, place(tok, width)]
    z_l[:, mine, :] = z_v[:, :, place(tok, width)]

    pl.semaphore_wait(barrier, group - 1)

    started = []

    def remote(src, dst, send_sem, recv_sem, device):
        copy = pltpu.make_async_remote_copy(
            src_ref=src, dst_ref=dst, send_sem=send_sem, recv_sem=recv_sem,
            device_id=device, device_id_type=MESH,
        )
        copy.start()
        started.append(copy)
        return copy

    partner = {"tok": tok + 1 - 2 * side}
    shared = (q_l, b_l, c_l, dt_l)
    gathered = {}

    def spread(kind, ref, index, at, device):
        part_at = ref.at[:, place(at, block), :]
        gathered[kind, index] = remote(
            part_at, part_at, gat_send.at[kind, index], gat_recv.at[kind, index], device
        )

    for o in range(1, lines):
        there = {"tok": lax.rem(line + o, lines) * 2 + side}
        for kind, ref in enumerate(shared):
            spread(kind, ref, o, tok, there)
    for kind, ref in enumerate(shared):
        spread(kind, ref, 0, tok, partner)

    first = {}

    def ship(kind, o, src, dst):
        first[kind, o] = remote(
            src, dst, send.at[kind, o], recv.at[kind, o], {"tok": lax.rem(tok + o, n_tok)}
        )

    for kind in range(3):
        for o in range(1, n_tok):
            to = lax.rem(tok + o, n_tok)
            src, dst = (
                (turn_v.at[:, :, place(to, width)], st_l.at[:, place(tok, cols), :]),
                (x_v.at[:, :, place(to, width)], x_l.at[:, mine, :]),
                (z_v.at[:, :, place(to, width)], z_l.at[:, mine, :]),
            )[kind]
            ship(kind, o, src, dst)

    for name in ("rate", "skip", "len", "acc"):
        held[name].wait()
    lane = iota((1, width), 1)
    rate_x = jnp.zeros((1, width), F32)
    skip_x = jnp.zeros((1, width), F32)
    for h in range(own):
        inside = (lane >= h * size) & (lane < (h + 1) * size)
        rate_x = jnp.where(inside, rate_ref[tok * own + h], rate_x)
        skip_x = jnp.where(inside, skip_ref[tok * own + h], skip_x)
    offset = iota((heads, width), 1) - (iota((heads, width), 0) - tok * own) * size
    pick = ((offset >= 0) & (offset < size)).astype(F32).astype(BF16)
    causal = iota((draft, draft), 0) >= iota((draft, draft), 1)
    lower = causal.astype(F32).astype(BF16)

    per = draft // group

    def targets(shape, dim):
        source = iota(shape, dim)
        target = jnp.zeros(shape, jnp.int32)
        for s in range(seqs):
            for g in range(group):
                start = s * draft + g * per
                base = (g % 2) * (rows // 2) + (g // 2) * each + s
                inside = (source >= start) & (source < start + per)
                target = jnp.where(inside, (source - start) * seqs + base, target)
        return target

    swap = (iota((rows, rows), 0) == targets((1, rows), 1)).astype(F32).astype(BF16)
    moved = targets((rows, 1), 0) == iota((rows, rows), 1)

    for o in range(1, lines):
        for kind, ref in enumerate(shared):
            gathered[kind, o].wait_recv()
            origin = lax.rem(line - o + lines, lines) * 2 + side
            spread(kind, ref, lines - 1 + o, origin, partner)
    gathered[0, 0].wait_recv()
    for o in range(1, lines):
        gathered[0, lines - 1 + o].wait_recv()
    for name in ("k", "v", "dk", "dv"):
        held[name].wait()
    scale = att ** (-0.5)
    m_rows = per_kv * draft
    big = iota((m_rows, m_rows), 0) == iota((m_rows, m_rows), 1)
    position = tok * cache + iota((1, cache), 1)
    draft_at = tok * block + iota((draft, block), 1)
    seen = draft_at <= iota((draft, block), 0)
    seen = jnp.concatenate([seen.astype(F32)] * per_kv, axis=0) > 0.5
    for s in range(seqs):
        q = jnp.concatenate([q_l[s, :, h * att : (h + 1) * att] for h in range(per_kv)], axis=0)
        old = lax.dot_general(q, k_v[s], NT, preferred_element_type=F32)
        old = jnp.where(position < len_ref[s], old, MASKED)
        new = lax.dot_general(q, dk_ref[s], NT, preferred_element_type=F32)
        new = jnp.where(seen, new, MASKED)
        peak = jnp.maximum(
            jnp.max(old, axis=1, keepdims=True), jnp.max(new, axis=1, keepdims=True)
        )
        peak = jnp.maximum(peak, FLOOR)
        old = jnp.exp((old - peak) * scale)
        new = jnp.exp((new - peak) * scale)
        total = jnp.sum(old, axis=1, keepdims=True) + jnp.sum(new, axis=1, keepdims=True)
        numer = dot(old.astype(BF16), v_v[s]) + dot(new.astype(BF16), dv_ref[s])
        safe = jnp.maximum(total, 1e-30)
        ctx = (numer / safe).astype(BF16)
        level = jnp.where(total > 0.0, peak * scale + jnp.log(safe), MASKED)
        for h in range(per_kv):
            n_s[s, h] = ctx[h * draft : (h + 1) * draft]
        stat_l[tok, s : s + 1, :] = jnp.sum(jnp.where(big, level, 0.0), axis=0, keepdims=True)
    for o in range(1, n_tok):
        to = lax.rem(tok + o, n_tok)
        ship(3, o, stat_l.at[tok], stat_l.at[tok])
        ship(4, o, n_s.at[:, :, place(to, block), :], n_l.at[tok])
    n_l[tok] = n_s[:, :, mine, :]

    for kind in range(1, len(shared)):
        for index in range(n_tok):
            if (kind, index) in gathered and not 1 <= index < lines:
                gathered[kind, index].wait_recv()
    for o in range(1, n_tok):
        first[0, o].wait_recv()
        first[1, o].wait_recv()
    saved = []
    for s in range(seqs):
        x = x_l[s].astype(F32)
        dtx = dot(dt_l[s], pick)
        run = -rate_x * dot(lower, dtx.astype(BF16))
        alive = iota((draft, width), 0) < acc_ref[s]
        end = -rate_x * jnp.sum(jnp.where(alive, dtx, 0.0), axis=0, keepdims=True)
        weight = jnp.where(alive, jnp.exp(jnp.where(alive, end - run, 0.0)) * dtx, 0.0)
        flow = b_l[s].astype(F32).T.astype(BF16)
        new = jnp.exp(end) * st_l[s].astype(F32) + dot(flow, (x * weight).astype(BF16))
        cm_s[s] = new.astype(BF16)
        saved.append((x, dtx, run))
    for o in range(1, n_tok):
        to = lax.rem(tok + o, n_tok)
        ship(5, o, cm_s.at[:, place(to, cols), :], cm_l.at[:, :, place(tok, width)])
    cm_l[:, :, place(tok, width)] = cm_s[:, place(tok, cols), :]

    for o in range(1, n_tok):
        first[2, o].wait_recv()
    held["gain"].wait()
    gated = []
    for s in range(seqs):
        x, dtx, run = saved[s]
        z = z_l[s].astype(F32)
        scaled = (x * dtx * jnp.exp(-run)).astype(BF16)
        mix = lax.dot_general(c_l[s], b_l[s], NT, preferred_element_type=F32)
        mix = jnp.where(causal, mix, 0.0).astype(BF16)
        y = jnp.exp(run) * (dot(mix, scaled) + dot(c_l[s], st_l[s])) + skip_x * x
        gated.append(y * z / (1.0 + jnp.exp(-z)))
    gated = jnp.concatenate(gated, axis=0)
    sums = jnp.sum(gated * gated, axis=1, keepdims=True)
    ss_l[me, 0:1, :] = jnp.sum(jnp.where(moved, sums, 0.0), axis=0, keepdims=True)
    squares = []
    for o in range(1, group):
        peer = lax.rem(me + o, group)
        squares.append(
            remote(
                ss_l.at[me], ss_l.at[me], ss_send.at[o], ss_recv.at[o],
                {"head": peer // n_tok, "tok": lax.rem(peer, n_tok)},
            )
        )
    gain = gain_ref[:, place(tok, width)]
    normed = dot(swap, (gated * gain).astype(BF16)).astype(BF16)

    held["w"].wait()
    tile = min(512, span)
    rs = {}
    pairs = []

    def forward(ch):
        pairs[ch].wait_recv()
        piece = pl.ds(ch * span, span)
        red[:, :, piece] = (
            part[side, :, :, piece].astype(F32) + pair_l[:, :, piece].astype(F32)
        ).astype(BF16)
        for o in range(1, half):
            peer = lax.rem(slot + o, half)
            rs[ch, o] = remote(
                red.at[peer, :, piece], rs_l.at[o, :, piece],
                rs_send.at[ch, o], rs_recv.at[ch, o],
                {"head": peer // lines, "tok": lax.rem(peer, lines) * 2 + side},
            )

    for ch in range(chunks):
        for start in range(ch * span, (ch + 1) * span, tile):
            val = dot(normed, w_v[:, start : start + tile]).astype(BF16)
            for p in range(2):
                for g in range(half):
                    at = (p * half + g) * each
                    part[p, g, :, start : start + tile] = val[at : at + each]
        piece = pl.ds(ch * span, span)
        pairs.append(
            remote(
                part.at[1 - side, :, :, piece], pair_l.at[:, :, piece],
                pair_send.at[ch], pair_recv.at[ch], partner,
            )
        )
        if ch > 0:
            forward(ch - 1)
    forward(chunks - 1)

    for o in range(1, n_tok):
        first[3, o].wait_recv()
        first[4, o].wait_recv()
    m_own = per_kv * block
    lanes = iota((m_own, m_rows), 1)
    r = iota((m_own, m_rows), 0)
    want = None
    for h in range(per_kv):
        t = r - h * block
        hit = (t >= 0) & (t < block) & (lanes == h * draft + tok * block + t)
        want = hit if want is None else want | hit
    for s in range(seqs):
        levels = [
            jnp.sum(jnp.where(want, stat_l[t][s : s + 1, :], 0.0), axis=1, keepdims=True)
            for t in range(n_tok)
        ]
        top = functools.reduce(jnp.maximum, levels)
        weights = [jnp.exp(level - top) for level in levels]
        den = functools.reduce(jnp.add, weights)
        acc = jnp.zeros((m_own, att), F32)
        for t in range(n_tok):
            got = jnp.concatenate([n_l[t, s, h].astype(F32) for h in range(per_kv)], axis=0)
            acc = acc + weights[t] * got
        acc = (acc / den).astype(BF16)
        for h in range(per_kv):
            ctx_ref[s, :, h * att : (h + 1) * att] = acc[h * block : (h + 1) * block]

    for o in range(1, n_tok):
        first[5, o].wait_recv()
    for s in range(seqs):
        for h in range(heads):
            com_ref[s, h] = cm_l[s, :, h * size : (h + 1) * size]

    for copy in squares:
        copy.wait_recv()
    base = side * (rows // 2) + slot * each
    here = iota((each, rows), 1) == base + iota((each, rows), 0)
    factors = []
    for o in range(half):
        origin = lax.rem(slot - o + half, half) // lines
        total = jnp.zeros((1, rows), F32)
        for t in range(n_tok):
            total = total + ss_l[origin * n_tok + t][0:1, :]
        column = jnp.sum(jnp.where(here, total, 0.0), axis=1, keepdims=True)
        factors.append(lax.rsqrt(column / (width * n_tok) + EPSILON))
    for ch in range(chunks):
        for o in range(1, half):
            rs[ch, o].wait_recv()
        for start in range(ch * span, (ch + 1) * span, tile):
            acc = red[slot, :, start : start + tile].astype(F32) * factors[0]
            for o in range(1, half):
                acc = acc + rs_l[o, :, start : start + tile].astype(F32) * factors[o]
            acc = acc.astype(BF16)
            for d in range(each // seqs):
                out_ref[d, :, start : start + tile] = acc[d * seqs : (d + 1) * seqs]

    for copy in started:
        copy.wait_send()


def finish(out_v, ctx_v, com_v, out_ref, ctx_ref, com_ref, sems):
    copies = [
        pltpu.make_async_copy(src, dst, sems.at[i])
        for i, (src, dst) in enumerate(((out_v, out_ref), (com_v, com_ref), (ctx_v, ctx_ref)))
    ]
    for copy in copies:
        copy.start()
    for copy in copies:
        copy.wait()


def body(
    mamba_input, gate_input, in_b, in_c, step_size, decay_rate, skip_weight, norm_gain,
    ssm_state, out_weight, queries, draft_token_keys, draft_values, cached_key_rows,
    cache_values, cache_len, accepted,
):
    n_tok = lax.axis_size("tok")
    n_head = lax.axis_size("head")
    group = n_head * n_tok
    seqs, block, features = mamba_input.shape
    heads = decay_rate.shape[0]
    size = features // heads
    cols = ssm_state.shape[3]
    state = cols * n_tok
    draft = block * n_tok
    width = features // n_tok
    att = draft_token_keys.shape[2]
    per_kv = queries.shape[2] // att
    cache = cached_key_rows.shape[1]
    out_cols = out_weight.shape[1]
    rows = seqs * draft
    each = rows // group
    chunks = 4
    half = group // 2
    turned = jnp.transpose(ssm_state, (0, 1, 3, 2))
    shapes = (
        (each // seqs, seqs, out_cols),
        (seqs, block, per_kv * att),
        (seqs, heads, cols, size),
    )
    operands = (
        mamba_input, gate_input, in_b, in_c, step_size, turned, queries, cached_key_rows,
        cache_values, out_weight, draft_token_keys, draft_values,
        norm_gain.reshape(1, features), decay_rate, skip_weight, cache_len, accepted,
    )
    vmem = pl.BlockSpec(memory_space=pltpu.VMEM)
    held = pl.pallas_call(
        functools.partial(kernel, (n_head, n_tok, seqs, block, heads, chunks)),
        out_shape=[pltpu.VMEM(shape, BF16) for shape in shapes],
        in_specs=[pl.BlockSpec(memory_space=pltpu.HBM)] * 17,
        out_specs=[vmem] * 3,
        scratch_shapes=[
            pltpu.VMEM((seqs, draft, width), BF16),
            pltpu.VMEM((seqs, draft, width), BF16),
            pltpu.VMEM((seqs, draft, state), BF16),
            pltpu.VMEM((seqs, draft, state), BF16),
            pltpu.VMEM((seqs, draft, heads), BF16),
            pltpu.VMEM((seqs, state, width), BF16),
            pltpu.VMEM((seqs, draft, per_kv * att), BF16),
            pltpu.VMEM((seqs, cache, att), BF16),
            pltpu.VMEM((seqs, cache, att), BF16),
            pltpu.VMEM(out_weight.shape, BF16),
            pltpu.VMEM((seqs, block, features), BF16),
            pltpu.VMEM((seqs, block, features), BF16),
            pltpu.VMEM((group, 1, rows), F32),
            pltpu.VMEM((seqs, state, width), BF16),
            pltpu.VMEM((seqs, cols, features), BF16),
            pltpu.VMEM((seqs, per_kv, draft, att), BF16),
            pltpu.VMEM((n_tok, seqs, per_kv, block, att), BF16),
            pltpu.VMEM((n_tok, seqs, per_kv * draft), F32),
            pltpu.VMEM((2, half, each, out_cols), BF16),
            pltpu.VMEM((half, each, out_cols), BF16),
            pltpu.VMEM((seqs, block, att), BF16),
            pltpu.VMEM((seqs, block, att), BF16),
            pltpu.VMEM((1, features), F32),
            pltpu.VMEM((seqs, heads, cols, size), BF16),
            pltpu.VMEM((seqs, cols, features), BF16),
            pltpu.VMEM((half, each, out_cols), BF16),
            pltpu.VMEM((half, each, out_cols), BF16),
            pltpu.SMEM(decay_rate.shape, F32),
            pltpu.SMEM(skip_weight.shape, F32),
            pltpu.SMEM(cache_len.shape, jnp.int32),
            pltpu.SMEM(accepted.shape, jnp.int32),
            pltpu.SemaphoreType.DMA((4, n_tok)),
            pltpu.SemaphoreType.DMA((4, n_tok)),
            pltpu.SemaphoreType.DMA((6, n_tok)),
            pltpu.SemaphoreType.DMA((6, n_tok)),
            pltpu.SemaphoreType.DMA((group,)),
            pltpu.SemaphoreType.DMA((group,)),
            pltpu.SemaphoreType.DMA((chunks, half)),
            pltpu.SemaphoreType.DMA((chunks, half)),
            pltpu.SemaphoreType.DMA((chunks,)),
            pltpu.SemaphoreType.DMA((chunks,)),
            pltpu.SemaphoreType.DMA((17,)),
        ],
        compiler_params=pltpu.CompilerParams(
            collective_id=0, has_side_effects=True, vmem_limit_bytes=40 * 1024 * 1024
        ),
        name="hybrid",
    )(*[pltpu.with_memory_space_constraint(a, pltpu.HBM) for a in operands])
    out, ctx, com = pl.pallas_call(
        finish,
        out_shape=[jax.ShapeDtypeStruct(shape, BF16) for shape in shapes],
        in_specs=[vmem] * 3,
        out_specs=[pl.BlockSpec(memory_space=pl.ANY)] * 3,
        scratch_shapes=[pltpu.SemaphoreType.DMA((3,))],
        compiler_params=pltpu.CompilerParams(vmem_limit_bytes=4 * 1024 * 1024),
        name="finish",
    )(*[pltpu.with_memory_space_constraint(a, pltpu.VMEM) for a in held])
    return (out, ctx, jnp.transpose(com, (0, 1, 3, 2)))


def solution(mesh):
    in_specs = (
        P("dp", "tok", "head"),
        P("dp", "tok", "head"),
        P("dp", "tok", "head"),
        P("dp", "tok", "head"),
        P("dp", "tok", "head"),
        P("head"),
        P("head"),
        P("head"),
        P("dp", "head", None, "tok"),
        P(("head", "tok"), None),
        P("dp", "tok", "head"),
        P("dp", "tok", "head"),
        P("dp", "tok", "head"),
        P("dp", "tok", "head"),
        P("dp", "tok", "head"),
        P("dp"),
        P("dp"),
    )
    out_specs = (
        P(("head", "tok"), "dp", None),
        P("dp", "tok", "head"),
        P("dp", "head", None, "tok"),
    )
    return jax.shard_map(body, mesh=mesh, in_specs=in_specs, out_specs=out_specs, check_vma=False)
```

```python
import functools
import jax
import jax.numpy as jnp
from jax import lax
from jax.experimental import pallas as pl
from jax.experimental.pallas import tpu as pltpu
from jax.sharding import PartitionSpec as P

EPSILON = 1e-05
MASKED = -1e30
FLOOR = -1e29
MESH = pl.DeviceIdType.MESH
F32 = jnp.float32
BF16 = jnp.bfloat16
NT = (((1,), (1,)), ((), ()))


def dot(a, b):
    return jnp.dot(a, b, preferred_element_type=F32)


def iota(shape, dim):
    return lax.broadcasted_iota(jnp.int32, shape, dim)


def kernel(
    dims,
    x_in, z_in, b_in, c_in, dt_in, st_in, q_in, k_in, v_in, w_in,
    dk_in, dv_in, gain_in, rate_in, skip_in, len_in, acc_in,
    out_ref, ctx_ref, com_ref,
    xz_v, xz_l, bc_l, dt_l, raw_v, turn_v, st_l, q_l, kv_v, new_v, w_v, gain_v,
    ss_l, cm_s, cm_l, n_s, n_l, stat_s, stat_l,
    part, pair_l, red, one_a, one_b, mid_a, mid_b, two_a, two_b,
    rate_ref, skip_ref, len_ref, acc_ref,
    sent, q_recv, bc_recv, dt_recv, st_recv, xz_recv, got, ss_recv,
    pair_recv, one_recv, two_recv, local,
):
    n_head, n_tok, seqs, block, heads, chunks = dims
    group = n_head * n_tok
    tok = lax.axis_index("tok")
    head = lax.axis_index("head")
    me = head * n_tok + tok
    draft = block * n_tok
    width = xz_l.shape[3]
    own = heads // n_tok
    size = width // own
    state = st_l.shape[1]
    cols = state // n_tok
    att = kv_v.shape[3]
    per_kv = q_l.shape[2] // att
    cache = kv_v.shape[2]
    per = draft // group
    out_cols = w_v.shape[1]
    span = out_cols // chunks
    half = group // 2
    side = lax.rem(tok, 2)
    line = tok // 2
    lines = n_tok // 2
    slot = head * lines + line

    def place(index, unit):
        return pl.ds(pl.multiple_of(index * unit, unit), unit)

    barrier = pltpu.get_barrier_semaphore()
    for o in range(1, group):
        peer = lax.rem(me + o, group)
        pl.semaphore_signal(
            barrier, inc=1,
            device_id={"head": peer // n_tok, "tok": lax.rem(peer, n_tok)},
            device_id_type=MESH,
        )

    def take(sem, ref):
        pltpu.make_async_copy(ref, ref, sem).wait()

    mine = place(tok, block)
    for sem, src, dst in (
        (0, st_in, raw_v),
        (1, q_in, q_l.at[:, mine, :]),
        (2, b_in, bc_l.at[0, :, mine, :]),
        (2, c_in, bc_l.at[1, :, mine, :]),
        (3, dt_in, dt_l.at[:, mine, :]),
        (4, x_in, xz_v.at[:, 0]),
        (4, z_in, xz_v.at[:, 1]),
        (5, dk_in, new_v.at[0]),
        (5, dv_in, new_v.at[1]),
        (6, k_in, kv_v.at[0]),
        (6, v_in, kv_v.at[1]),
        (7, len_in, len_ref),
        (8, acc_in, acc_ref),
        (9, rate_in, rate_ref),
        (10, skip_in, skip_ref),
        (11, gain_in, gain_v),
        (12, w_in, w_v),
    ):
        pltpu.make_async_copy(src, dst, local.at[sem]).start()

    take(local.at[0], raw_v)
    for s in range(seqs):
        turn_v[s] = jnp.concatenate(
            [raw_v[s, h].astype(F32) for h in range(heads)], axis=1
        ).astype(BF16)
    st_l[:, place(tok, cols), :] = turn_v[:, :, place(tok, width)]
    take(local.at[1], q_l.at[:, mine, :])
    take(local.at[2], bc_l.at[:, :, mine, :])
    take(local.at[3], dt_l.at[:, mine, :])
    take(local.at[4], xz_v)
    xz_l[:, :, mine, :] = xz_v[:, :, :, place(tok, width)]

    pl.semaphore_wait(barrier, group - 1)

    def remote(kind, src, dst, recv_sem, device):
        pltpu.make_async_remote_copy(
            src_ref=src, dst_ref=dst, send_sem=sent.at[kind], recv_sem=recv_sem,
            device_id=device, device_id_type=MESH,
        ).start()

    flip = tok + 1 - 2 * side
    partner = {"tok": flip}

    def share(at, device, q_sem, sem, only=None):
        span_at = place(at, block)
        for kind, ref, recv in (
            (0, q_l.at[:, span_at, :], q_recv.at[q_sem]),
            (1, bc_l.at[:, :, span_at, :], bc_recv.at[sem]),
            (2, dt_l.at[:, span_at, :], dt_recv.at[sem]),
        ):
            if only is None or kind in only:
                remote(kind, ref, ref, recv, device)

    for o in range(1, lines):
        share(tok, {"tok": lax.rem(line + o, lines) * 2 + side}, o, o)
    share(tok, partner, 0, 0)
    for s in range(seqs):
        for o in range(1, n_tok):
            to = lax.rem(tok + o, n_tok)
            remote(
                3, turn_v.at[s, :, place(to, width)], st_l.at[s, place(tok, cols), :],
                st_recv.at[s], {"tok": to},
            )
        for o in range(1, n_tok):
            to = lax.rem(tok + o, n_tok)
            remote(
                4, xz_v.at[s, :, :, place(to, width)], xz_l.at[s, :, mine, :],
                xz_recv.at[s], {"tok": to},
            )

    for i, ref in ((7, len_ref), (8, acc_ref), (9, rate_ref), (10, skip_ref)):
        take(local.at[i], ref)
    take(local.at[5], new_v)
    take(local.at[6], kv_v)
    scale = att ** (-0.5)
    m_own = per_kv * block
    eye = iota((m_own, m_own), 0) == iota((m_own, m_own), 1)
    position = tok * cache + iota((1, cache), 1)
    inner = iota((block, block), 1) - iota((block, block), 0)
    inner = jnp.concatenate([inner] * per_kv, axis=0)

    def attend(t, n_to, stat_to):
        for s in range(seqs):
            q = jnp.concatenate(
                [q_l[s, place(t, block), h * att : (h + 1) * att] for h in range(per_kv)], axis=0
            )
            old = lax.dot_general(q, kv_v[0, s], NT, preferred_element_type=F32)
            old = jnp.where(position < len_ref[s], old, MASKED)
            new = lax.dot_general(q, new_v[0, s], NT, preferred_element_type=F32)
            new = jnp.where(inner <= (t - tok) * block, new, MASKED)
            peak = jnp.maximum(
                jnp.max(old, axis=1, keepdims=True), jnp.max(new, axis=1, keepdims=True)
            )
            peak = jnp.maximum(peak, FLOOR)
            old = jnp.exp((old - peak) * scale)
            new = jnp.exp((new - peak) * scale)
            total = jnp.sum(old, axis=1, keepdims=True) + jnp.sum(new, axis=1, keepdims=True)
            numer = dot(old.astype(BF16), kv_v[1, s]) + dot(new.astype(BF16), new_v[1, s])
            safe = jnp.maximum(total, 1e-30)
            level = jnp.where(total > 0.0, peak * scale + jnp.log(safe), MASKED)
            n_to[s] = (numer / safe).astype(BF16)
            stat_to[s : s + 1, :] = jnp.sum(jnp.where(eye, level, 0.0), axis=0, keepdims=True)

    def attend_for(t, index):
        attend(t, n_s.at[index], stat_s.at[index])
        remote(5, n_s.at[index], n_l.at[tok], got.at[0], {"tok": t})
        remote(6, stat_s.at[index], stat_l.at[tok], got.at[1], {"tok": t})

    attend(tok, n_l.at[tok], stat_l.at[tok])
    take(q_recv.at[0], q_l.at[:, mine, :])
    attend_for(flip, 0)
    for o in range(1, lines):
        origin = lax.rem(line - o + lines, lines) * 2 + side
        take(q_recv.at[o], q_l.at[:, mine, :])
        share(origin, partner, lines - 1 + o, 0, (0,))
    for o in range(1, lines):
        origin = lax.rem(line - o + lines, lines) * 2 + side
        take(bc_recv.at[o], bc_l.at[:, :, mine, :])
        take(dt_recv.at[o], dt_l.at[:, mine, :])
        share(origin, partner, 0, 0, (1, 2))
    for o in range(1, lines):
        attend_for(lax.rem(line - o + lines, lines) * 2 + side, o)
    for o in range(1, lines):
        take(q_recv.at[lines - 1 + o], q_l.at[:, mine, :])
        attend_for(lax.rem(line - o + lines, lines) * 2 + 1 - side, lines - 1 + o)

    lane = iota((1, width), 1)
    rate_x = jnp.zeros((1, width), F32)
    skip_x = jnp.zeros((1, width), F32)
    for h in range(own):
        inside = (lane >= h * size) & (lane < (h + 1) * size)
        rate_x = jnp.where(inside, rate_ref[tok * own + h], rate_x)
        skip_x = jnp.where(inside, skip_ref[tok * own + h], skip_x)
    offset = iota((heads, width), 1) - (iota((heads, width), 0) - tok * own) * size
    pick = ((offset >= 0) & (offset < size)).astype(F32).astype(BF16)
    causal = iota((draft, draft), 0) >= iota((draft, draft), 1)
    lower = causal.astype(F32).astype(BF16)

    def target(dim):
        source = iota((draft, draft), dim)
        result = jnp.zeros((draft, draft), jnp.int32)
        for g in range(group):
            base = (g % 2) * (draft // 2) + (g // 2) * per
            inside = (source >= g * per) & (source < (g + 1) * per)
            result = jnp.where(inside, source - g * per + base, result)
        return result

    swap = (iota((draft, draft), 0) == target(1)).astype(F32).astype(BF16)
    moved = target(0) == iota((draft, draft), 1)
    take(local.at[11], gain_v)
    gain = gain_v[:, place(tok, width)]
    take(local.at[12], w_v)
    take(bc_recv.at[0], bc_l.at[:, :, pl.ds(0, lines * block), :])
    take(dt_recv.at[0], dt_l.at[:, pl.ds(0, lines * block), :])

    tile = min(512, span)

    def piece_of(ch):
        return pl.ds(ch * span, span)

    def mix_tokens(s):
        x = xz_l[s, 0].astype(F32)
        z = xz_l[s, 1].astype(F32)
        dtx = dot(dt_l[s], pick)
        run = -rate_x * dot(lower, dtx.astype(BF16))
        scaled = (x * dtx * jnp.exp(-run)).astype(BF16)
        mix = lax.dot_general(bc_l[1, s], bc_l[0, s], NT, preferred_element_type=F32)
        mix = jnp.where(causal, mix, 0.0).astype(BF16)
        y = jnp.exp(run) * (dot(mix, scaled) + dot(bc_l[1, s], st_l[s])) + skip_x * x
        gated = y * z / (1.0 + jnp.exp(-z))
        sums = jnp.sum(gated * gated, axis=1, keepdims=True)
        ss_l[s, me] = jnp.sum(jnp.where(moved, sums, 0.0), axis=0, keepdims=True)
        for o in range(1, group):
            peer = lax.rem(me + o, group)
            remote(
                7, ss_l.at[s, me], ss_l.at[s, me], ss_recv.at[s],
                {"head": peer // n_tok, "tok": lax.rem(peer, n_tok)},
            )
        return dot(swap, (gated * gain).astype(BF16)).astype(BF16), (x, dtx, run)

    def project(s, normed):
        for ch in range(chunks):
            for start in range(ch * span, (ch + 1) * span, tile):
                val = dot(normed, w_v[:, start : start + tile])
                for p in range(2):
                    for g in range(half):
                        at = (p * half + g) * per
                        part[s, p, g // lines, g % lines, :, start : start + tile] = val[
                            at : at + per
                        ].astype(BF16)
            remote(
                8, part.at[s, 1 - side, :, :, :, piece_of(ch)],
                pair_l.at[s, :, :, :, piece_of(ch)], pair_recv.at[s, ch], partner,
            )

    def commit(s, saved):
        x, dtx, run = saved
        alive = iota((draft, width), 0) < acc_ref[s]
        end = -rate_x * jnp.sum(jnp.where(alive, dtx, 0.0), axis=0, keepdims=True)
        weight = jnp.where(alive, jnp.exp(jnp.where(alive, end - run, 0.0)) * dtx, 0.0)
        flow = bc_l[0, s].astype(F32).T.astype(BF16)
        new = jnp.exp(end) * st_l[s].astype(F32) + dot(flow, (x * weight).astype(BF16))
        cm_s[s] = new.astype(BF16)
        for o in range(1, n_tok):
            to = lax.rem(tok + o, n_tok)
            remote(
                9, cm_s.at[s, place(to, cols), :], cm_l.at[s, :, place(tok, width)],
                got.at[2], {"tok": to},
            )
        cm_l[s, :, place(tok, width)] = cm_s[s, place(tok, cols), :]

    def line_first(ch):
        return ch % 2 == 0

    def forward(s, ch):
        piece = piece_of(ch)
        take(pair_recv.at[s, ch], pair_l.at[s, :, :, :, piece])
        red[s, :, :, :, piece] = (
            part[s, side, :, :, :, piece].astype(F32) + pair_l[s, :, :, :, piece].astype(F32)
        ).astype(BF16)
        if line_first(ch):
            for o in range(1, lines):
                to = lax.rem(line + o, lines)
                remote(
                    10, red.at[s, :, to, :, piece], one_a.at[s, o, :, :, piece],
                    one_recv.at[s, ch, o - 1], {"tok": to * 2 + side},
                )
        else:
            for o in range(1, n_head):
                to = lax.rem(head + o, n_head)
                remote(
                    11, red.at[s, to, :, :, piece], one_b.at[s, o, :, :, piece],
                    one_recv.at[s, ch, o - 1], {"head": to},
                )

    def factor(s, origin, base, count):
        total = jnp.zeros((1, draft), F32)
        for t in range(n_tok):
            total = total + ss_l[s, origin * n_tok + t]
        here = iota((count, draft), 1) == base + iota((count, draft), 0)
        column = jnp.sum(jnp.where(here, total, 0.0), axis=1, keepdims=True)
        return lax.rsqrt(column / (width * n_tok) + EPSILON)

    def second(s, ch, factors):
        piece = piece_of(ch)
        if line_first(ch):
            for o in range(1, lines):
                take(one_recv.at[s, ch, o - 1], one_a.at[s, o, :, :, piece])
            total = red[s, :, line, :, piece].astype(F32)
            for o in range(1, lines):
                total = total + one_a[s, o, :, :, piece].astype(F32)
            mid_a[s, :, :, piece] = total.astype(BF16)
            for o in range(1, n_head):
                to = lax.rem(head + o, n_head)
                remote(
                    12, mid_a.at[s, to, :, piece], two_a.at[s, o, :, piece],
                    two_recv.at[s, ch, o - 1], {"head": to},
                )
        else:
            for o in range(1, n_head):
                take(one_recv.at[s, ch, o - 1], one_b.at[s, o, :, :, piece])
            for l in range(lines):
                near = slice(l * per, (l + 1) * per)
                total = red[s, head, l, :, piece].astype(F32) * factors[0][near]
                for o in range(1, n_head):
                    total = total + one_b[s, o, l, :, piece].astype(F32) * factors[o][near]
                mid_b[s, l, :, piece] = total.astype(BF16)
            for o in range(1, lines):
                to = lax.rem(line + o, lines)
                remote(
                    13, mid_b.at[s, to, :, piece], two_b.at[s, o, :, piece],
                    two_recv.at[s, ch, o - 1], {"tok": to * 2 + side},
                )

    def final(s, ch, factors):
        piece = piece_of(ch)
        if line_first(ch):
            for o in range(1, n_head):
                take(two_recv.at[s, ch, o - 1], two_a.at[s, o, :, piece])
            total = mid_a[s, head, :, piece].astype(F32) * factors[0]
            for o in range(1, n_head):
                total = total + two_a[s, o, :, piece].astype(F32) * factors[o]
        else:
            for o in range(1, lines):
                take(two_recv.at[s, ch, o - 1], two_b.at[s, o, :, piece])
            total = mid_b[s, line, :, piece].astype(F32)
            for o in range(1, lines):
                total = total + two_b[s, o, :, piece].astype(F32)
        return total

    for s in range(seqs):
        take(st_recv.at[s], st_l.at[s, pl.ds(0, (n_tok - 1) * cols), :])
        take(xz_recv.at[s], xz_l.at[s, :, pl.ds(0, (n_tok - 1) * block), :])
        normed, saved = mix_tokens(s)
        project(s, normed)
        commit(s, saved)
        for ch in range(chunks):
            forward(s, ch)

    take(got.at[0], n_l.at[pl.ds(0, n_tok - 1)])
    take(got.at[1], stat_l.at[pl.ds(0, n_tok - 1)])
    for s in range(seqs):
        levels = [
            jnp.sum(jnp.where(eye, stat_l[t, s : s + 1, :], 0.0), axis=1, keepdims=True)
            for t in range(n_tok)
        ]
        top = functools.reduce(jnp.maximum, levels)
        weights = [jnp.exp(level - top) for level in levels]
        den = functools.reduce(jnp.add, weights)
        acc = jnp.zeros((m_own, att), F32)
        for t in range(n_tok):
            acc = acc + weights[t] * n_l[t, s].astype(F32)
        acc = (acc / den).astype(BF16)
        for h in range(per_kv):
            ctx_ref[s, :, h * att : (h + 1) * att] = acc[h * block : (h + 1) * block]

    ours = side * (draft // 2) + head * lines * per
    narrow = []
    for s in range(seqs):
        take(ss_recv.at[s], ss_l.at[s, pl.ds(0, group - 1)])
        origins = [lax.rem(head - o + n_head, n_head) for o in range(n_head)]
        wide = [factor(s, origin, ours, lines * per) for origin in origins]
        narrow.append([factor(s, origin, ours + line * per, per) for origin in origins])
        for ch in range(chunks):
            second(s, ch, wide)

    take(got.at[2], cm_l.at[:, :, pl.ds(0, (n_tok - 1) * width)])
    for s in range(seqs):
        for h in range(heads):
            com_ref[s, h] = cm_l[s, :, h * size : (h + 1) * size]

    at, of = iota((per * seqs, per * seqs), 0), iota((per * seqs, per * seqs), 1)
    weave = jnp.zeros((per * seqs, per * seqs), F32)
    for s in range(seqs):
        weave = jnp.where(at == (of - s * per) * seqs + s, jnp.where((of >= s * per) & (of < (s + 1) * per), 1.0, weave), weave)
    weave = weave.astype(BF16)
    for ch in range(chunks):
        both = jnp.concatenate([final(s, ch, narrow[s]) for s in range(seqs)], axis=0)
        both = dot(weave, both.astype(BF16)).astype(BF16)
        for d in range(per):
            out_ref[d, :, piece_of(ch)] = both[d * seqs : (d + 1) * seqs]

    others = pl.ds(0, n_tok - 1)
    most = pl.ds(0, (n_tok - 1) * block)
    take(sent.at[0], q_l.at[:, most, :])
    take(sent.at[1], bc_l.at[:, :, most, :])
    take(sent.at[2], dt_l.at[:, most, :])
    take(sent.at[3], turn_v.at[:, :, pl.ds(0, (n_tok - 1) * width)])
    take(sent.at[4], xz_v.at[:, :, :, pl.ds(0, (n_tok - 1) * width)])
    take(sent.at[5], n_s.at[others])
    take(sent.at[6], stat_s.at[others])
    take(sent.at[7], ss_l.at[:, pl.ds(0, group - 1)])
    take(sent.at[8], pair_l)
    take(sent.at[9], cm_s.at[:, pl.ds(0, (n_tok - 1) * cols), :])
    partial = pl.ds(0, out_cols // 2)
    take(sent.at[10], one_a.at[:, pl.ds(1, lines - 1), :, :, partial])
    take(sent.at[11], one_b.at[:, pl.ds(1, n_head - 1), :, :, partial])
    take(sent.at[12], two_a.at[:, pl.ds(1, n_head - 1), :, partial])
    take(sent.at[13], two_b.at[:, pl.ds(1, lines - 1), :, partial])


def finish(out_v, ctx_v, com_v, out_ref, ctx_ref, com_ref, sems):
    copies = [
        pltpu.make_async_copy(src, dst, sems.at[i])
        for i, (src, dst) in enumerate(((out_v, out_ref), (com_v, com_ref), (ctx_v, ctx_ref)))
    ]
    for copy in copies:
        copy.start()
    for copy in copies:
        copy.wait()


def body(
    mamba_input, gate_input, in_b, in_c, step_size, decay_rate, skip_weight, norm_gain,
    ssm_state, out_weight, queries, draft_token_keys, draft_values, cached_key_rows,
    cache_values, cache_len, accepted,
):
    n_tok = lax.axis_size("tok")
    n_head = lax.axis_size("head")
    group = n_head * n_tok
    lines = n_tok // 2
    seqs, block, features = mamba_input.shape
    heads = decay_rate.shape[0]
    size = features // heads
    cols = ssm_state.shape[3]
    state = cols * n_tok
    draft = block * n_tok
    width = features // n_tok
    att = draft_token_keys.shape[2]
    per_kv = queries.shape[2] // att
    cache = cached_key_rows.shape[1]
    out_cols = out_weight.shape[1]
    per = draft // group
    chunks = 4
    hops = max(lines, n_head) - 1
    turned = jnp.transpose(ssm_state, (0, 1, 3, 2))
    shapes = (
        (per, seqs, out_cols),
        (seqs, block, per_kv * att),
        (seqs, heads, cols, size),
    )
    operands = (
        mamba_input, gate_input, in_b, in_c, step_size, turned, queries, cached_key_rows,
        cache_values, out_weight, draft_token_keys, draft_values,
        norm_gain.reshape(1, features), decay_rate, skip_weight, cache_len, accepted,
    )
    vmem = pl.BlockSpec(memory_space=pltpu.VMEM)
    held = pl.pallas_call(
        functools.partial(kernel, (n_head, n_tok, seqs, block, heads, chunks)),
        out_shape=[pltpu.VMEM(shape, BF16) for shape in shapes],
        in_specs=[pl.BlockSpec(memory_space=pltpu.HBM)] * len(operands),
        out_specs=[vmem] * 3,
        scratch_shapes=[
            pltpu.VMEM((seqs, 2, block, features), BF16),
            pltpu.VMEM((seqs, 2, draft, width), BF16),
            pltpu.VMEM((2, seqs, draft, state), BF16),
            pltpu.VMEM((seqs, draft, heads), BF16),
            pltpu.VMEM((seqs, heads, cols, size), BF16),
            pltpu.VMEM((seqs, cols, features), BF16),
            pltpu.VMEM((seqs, state, width), BF16),
            pltpu.VMEM((seqs, draft, per_kv * att), BF16),
            pltpu.VMEM((2, seqs, cache, att), BF16),
            pltpu.VMEM((2, seqs, block, att), BF16),
            pltpu.VMEM(out_weight.shape, BF16),
            pltpu.VMEM((1, features), F32),
            pltpu.VMEM((seqs, group, 1, draft), F32),
            pltpu.VMEM((seqs, state, width), BF16),
            pltpu.VMEM((seqs, cols, features), BF16),
            pltpu.VMEM((n_tok, seqs, per_kv * block, att), BF16),
            pltpu.VMEM((n_tok, seqs, per_kv * block, att), BF16),
            pltpu.VMEM((n_tok, seqs, per_kv * block), F32),
            pltpu.VMEM((n_tok, seqs, per_kv * block), F32),
            pltpu.VMEM((seqs, 2, n_head, lines, per, out_cols), BF16),
            pltpu.VMEM((seqs, n_head, lines, per, out_cols), BF16),
            pltpu.VMEM((seqs, n_head, lines, per, out_cols), BF16),
            pltpu.VMEM((seqs, lines, n_head, per, out_cols), BF16),
            pltpu.VMEM((seqs, n_head, lines, per, out_cols), BF16),
            pltpu.VMEM((seqs, n_head, per, out_cols), BF16),
            pltpu.VMEM((seqs, lines, per, out_cols), BF16),
            pltpu.VMEM((seqs, n_head, per, out_cols), BF16),
            pltpu.VMEM((seqs, lines, per, out_cols), BF16),
            pltpu.SMEM(decay_rate.shape, F32),
            pltpu.SMEM(skip_weight.shape, F32),
            pltpu.SMEM(cache_len.shape, jnp.int32),
            pltpu.SMEM(accepted.shape, jnp.int32),
            pltpu.SemaphoreType.DMA((14,)),
            pltpu.SemaphoreType.DMA((n_tok - 1,)),
            pltpu.SemaphoreType.DMA((lines,)),
            pltpu.SemaphoreType.DMA((lines,)),
            pltpu.SemaphoreType.DMA((seqs,)),
            pltpu.SemaphoreType.DMA((seqs,)),
            pltpu.SemaphoreType.DMA((3,)),
            pltpu.SemaphoreType.DMA((seqs,)),
            pltpu.SemaphoreType.DMA((seqs, chunks)),
            pltpu.SemaphoreType.DMA((seqs, chunks, hops)),
            pltpu.SemaphoreType.DMA((seqs, chunks, hops)),
            pltpu.SemaphoreType.DMA((13,)),
        ],
        compiler_params=pltpu.CompilerParams(
            collective_id=0, has_side_effects=True, vmem_limit_bytes=40 * 1024 * 1024
        ),
        name="hybrid",
    )(*[pltpu.with_memory_space_constraint(a, pltpu.HBM) for a in operands])
    out, ctx, com = pl.pallas_call(
        finish,
        out_shape=[jax.ShapeDtypeStruct(shape, BF16) for shape in shapes],
        in_specs=[vmem] * 3,
        out_specs=[pl.BlockSpec(memory_space=pl.ANY)] * 3,
        scratch_shapes=[pltpu.SemaphoreType.DMA((3,))],
        compiler_params=pltpu.CompilerParams(vmem_limit_bytes=4 * 1024 * 1024),
        name="finish",
    )(*[pltpu.with_memory_space_constraint(a, pltpu.VMEM) for a in held])
    return (out, ctx, jnp.transpose(com, (0, 1, 3, 2)))


def solution(mesh):
    in_specs = (
        P("dp", "tok", "head"),
        P("dp", "tok", "head"),
        P("dp", "tok", "head"),
        P("dp", "tok", "head"),
        P("dp", "tok", "head"),
        P("head"),
        P("head"),
        P("head"),
        P("dp", "head", None, "tok"),
        P(("head", "tok"), None),
        P("dp", "tok", "head"),
        P("dp", "tok", "head"),
        P("dp", "tok", "head"),
        P("dp", "tok", "head"),
        P("dp", "tok", "head"),
        P("dp"),
        P("dp"),
    )
    out_specs = (
        P(("head", "tok"), "dp", None),
        P("dp", "tok", "head"),
        P("dp", "head", None, "tok"),
    )
    return jax.shard_map(body, mesh=mesh, in_specs=in_specs, out_specs=out_specs, check_vma=False)
```

```python
import functools
import jax
import jax.numpy as jnp
from jax import lax
from jax.experimental import pallas as pl
from jax.experimental.pallas import tpu as pltpu
from jax.sharding import PartitionSpec as P

EPSILON = 1e-05
MASKED = -1e30
FLOOR = -1e29
MESH = pl.DeviceIdType.MESH
F32 = jnp.float32
BF16 = jnp.bfloat16
NT = (((1,), (1,)), ((), ()))


def dot(a, b):
    return jnp.dot(a, b, preferred_element_type=F32)


def iota(shape, dim):
    return lax.broadcasted_iota(jnp.int32, shape, dim)


def kernel(
    dims,
    x_in, z_in, b_in, c_in, dt_in, st_in, q_in, k_in, v_in, w_in,
    dk_in, dv_in, gain_in, rate_in, skip_in, len_in, acc_in,
    out_ref, ctx_ref, com_ref,
    xz_v, xz_l, bc_l, dt_l, raw_v, turn_v, st_l, q_l, kv_v, new_v, w_v, gain_v,
    ss_l, cm_s, cm_l, n_s, n_l, stat_s, stat_l,
    part, pair_l, red, one_a, one_b, mid_a, mid_b, two_a, two_b,
    rate_ref, skip_ref, len_ref, acc_ref,
    sent, q_recv, bc_recv, dt_recv, st_recv, xz_recv, got, ss_recv,
    pair_recv, one_recv, two_recv, local,
):
    n_head, n_tok, seqs, block, heads, chunks = dims
    group = n_head * n_tok
    tok = lax.axis_index("tok")
    head = lax.axis_index("head")
    me = head * n_tok + tok
    draft = block * n_tok
    width = xz_l.shape[3]
    own = heads // n_tok
    size = width // own
    state = st_l.shape[1]
    cols = state // n_tok
    att = kv_v.shape[3]
    per_kv = q_l.shape[2] // att
    cache = kv_v.shape[2]
    per = draft // group
    out_cols = w_v.shape[1]
    span = out_cols // chunks
    half = group // 2
    side = lax.rem(tok, 2)
    line = tok // 2
    lines = n_tok // 2
    slot = head * lines + line

    def place(index, unit):
        return pl.ds(pl.multiple_of(index * unit, unit), unit)

    barrier = pltpu.get_barrier_semaphore()
    for o in range(1, group):
        peer = lax.rem(me + o, group)
        pl.semaphore_signal(
            barrier, inc=1,
            device_id={"head": peer // n_tok, "tok": lax.rem(peer, n_tok)},
            device_id_type=MESH,
        )

    def take(sem, ref):
        pltpu.make_async_copy(ref, ref, sem).wait()

    mine = place(tok, block)
    for sem, src, dst in (
        (0, st_in, raw_v),
        (1, q_in, q_l.at[:, mine, :]),
        (2, b_in, bc_l.at[0, :, mine, :]),
        (2, c_in, bc_l.at[1, :, mine, :]),
        (3, dt_in, dt_l.at[:, mine, :]),
        (4, x_in, xz_v.at[:, 0]),
        (4, z_in, xz_v.at[:, 1]),
        (5, dk_in, new_v.at[0]),
        (5, dv_in, new_v.at[1]),
        (6, k_in, kv_v.at[0]),
        (6, v_in, kv_v.at[1]),
        (7, len_in, len_ref),
        (8, acc_in, acc_ref),
        (9, rate_in, rate_ref),
        (10, skip_in, skip_ref),
        (11, gain_in, gain_v),
        (12, w_in, w_v),
    ):
        pltpu.make_async_copy(src, dst, local.at[sem]).start()

    take(local.at[0], raw_v)
    for s in range(seqs):
        turn_v[s] = jnp.concatenate(
            [raw_v[s, h].astype(F32) for h in range(heads)], axis=1
        ).astype(BF16)
    st_l[:, place(tok, cols), :] = turn_v[:, :, place(tok, width)]
    take(local.at[1], q_l.at[:, mine, :])
    take(local.at[2], bc_l.at[:, :, mine, :])
    take(local.at[3], dt_l.at[:, mine, :])
    take(local.at[4], xz_v)
    xz_l[:, :, mine, :] = xz_v[:, :, :, place(tok, width)]

    pl.semaphore_wait(barrier, group - 1)

    def remote(kind, src, dst, recv_sem, device):
        pltpu.make_async_remote_copy(
            src_ref=src, dst_ref=dst, send_sem=sent.at[kind], recv_sem=recv_sem,
            device_id=device, device_id_type=MESH,
        ).start()

    flip = tok + 1 - 2 * side
    partner = {"tok": flip}

    def share(at, device, q_sem, sem, only=None):
        span_at = place(at, block)
        for kind, ref, recv in (
            (0, q_l.at[:, span_at, :], q_recv.at[q_sem]),
            (1, bc_l.at[:, :, span_at, :], bc_recv.at[sem]),
            (2, dt_l.at[:, span_at, :], dt_recv.at[sem]),
        ):
            if only is None or kind in only:
                remote(kind, ref, ref, recv, device)

    def across(o):
        return lax.rem(line + o, lines) * 2 + lax.rem(side + o, 2)

    def origin(o, near):
        return lax.rem(line - o + lines, lines) * 2 + lax.rem(near + o, 2)

    for o in range(1, lines):
        share(tok, {"tok": across(o)}, o, o)
    share(tok, partner, 0, 0)
    for s in range(seqs):
        for o in range(1, n_tok):
            to = lax.rem(tok + o, n_tok)
            remote(
                3, turn_v.at[s, :, place(to, width)], st_l.at[s, place(tok, cols), :],
                st_recv.at[s], {"tok": to},
            )
        for o in range(1, n_tok):
            to = lax.rem(tok + o, n_tok)
            remote(
                4, xz_v.at[s, :, :, place(to, width)], xz_l.at[s, :, mine, :],
                xz_recv.at[s], {"tok": to},
            )

    for i, ref in ((7, len_ref), (8, acc_ref), (9, rate_ref), (10, skip_ref)):
        take(local.at[i], ref)
    take(local.at[5], new_v)
    take(local.at[6], kv_v)
    scale = att ** (-0.5)
    pair = 2 * block
    m_own = per_kv * block
    m_pair = per_kv * pair
    eye = iota((m_pair, m_pair), 0) == iota((m_pair, m_pair), 1)
    position = tok * cache + iota((1, cache), 1)
    inner = iota((pair, block), 1) - iota((pair, block), 0)
    inner = jnp.concatenate([inner] * per_kv, axis=0)

    def attend(at):
        for s in range(seqs):
            q = jnp.concatenate(
                [q_l[s, place(at, pair), h * att : (h + 1) * att] for h in range(per_kv)], axis=0
            )
            old = lax.dot_general(q, kv_v[0, s], NT, preferred_element_type=F32)
            old = jnp.where(position < len_ref[s], old, MASKED)
            new = lax.dot_general(q, new_v[0, s], NT, preferred_element_type=F32)
            new = jnp.where(inner <= at * pair - tok * block, new, MASKED)
            peak = jnp.maximum(
                jnp.max(old, axis=1, keepdims=True), jnp.max(new, axis=1, keepdims=True)
            )
            peak = jnp.maximum(peak, FLOOR)
            old = jnp.exp((old - peak) * scale)
            new = jnp.exp((new - peak) * scale)
            total = jnp.sum(old, axis=1, keepdims=True) + jnp.sum(new, axis=1, keepdims=True)
            numer = dot(old.astype(BF16), kv_v[1, s]) + dot(new.astype(BF16), new_v[1, s])
            safe = jnp.maximum(total, 1e-30)
            level = jnp.where(total > 0.0, peak * scale + jnp.log(safe), MASKED)
            ctx = (numer / safe).astype(BF16)
            for c in range(2):
                for h in range(per_kv):
                    n_s[at * 2 + c, s, h * block : (h + 1) * block] = ctx[
                        (h * 2 + c) * block : (h * 2 + c + 1) * block
                    ]
            stat_s[at, s : s + 1, :] = jnp.sum(jnp.where(eye, level, 0.0), axis=0, keepdims=True)

    def answer(t):
        remote(5, n_s.at[t], n_l.at[tok], got.at[0], {"tok": t})
        remote(6, stat_s.at[t // 2], stat_l.at[tok], got.at[1], {"tok": t})

    take(q_recv.at[0], q_l.at[:, mine, :])
    attend(line)
    answer(flip)
    n_l[tok] = n_s[tok]
    stat_l[tok] = stat_s[line]
    for o in range(1, lines):
        take(q_recv.at[o], q_l.at[:, mine, :])
        share(origin(o, side), partner, lines - 1 + o, 0, (0,))
    for o in range(1, lines):
        take(bc_recv.at[o], bc_l.at[:, :, mine, :])
        take(dt_recv.at[o], dt_l.at[:, mine, :])
        share(origin(o, side), partner, 0, 0, (1, 2))
    for o in range(1, lines):
        take(q_recv.at[lines - 1 + o], q_l.at[:, mine, :])
        attend(lax.rem(line - o + lines, lines))
        answer(origin(o, side))
        answer(origin(o, 1 - side))

    lane = iota((1, width), 1)
    rate_x = jnp.zeros((1, width), F32)
    skip_x = jnp.zeros((1, width), F32)
    for h in range(own):
        inside = (lane >= h * size) & (lane < (h + 1) * size)
        rate_x = jnp.where(inside, rate_ref[tok * own + h], rate_x)
        skip_x = jnp.where(inside, skip_ref[tok * own + h], skip_x)
    offset = iota((heads, width), 1) - (iota((heads, width), 0) - tok * own) * size
    pick = ((offset >= 0) & (offset < size)).astype(F32).astype(BF16)
    causal = iota((draft, draft), 0) >= iota((draft, draft), 1)
    lower = causal.astype(F32).astype(BF16)

    level_eye = iota((draft, draft), 0) == iota((draft, draft), 1)
    take(local.at[11], gain_v)
    gain = gain_v[:, place(tok, width)]
    take(local.at[12], w_v)
    take(bc_recv.at[0], bc_l.at[:, :, pl.ds(0, lines * block), :])
    take(dt_recv.at[0], dt_l.at[:, pl.ds(0, lines * block), :])
    early = []
    for s in range(seqs):
        dtx = dot(dt_l[s], pick)
        run = -rate_x * dot(lower, dtx.astype(BF16))
        mix = lax.dot_general(bc_l[1, s], bc_l[0, s], NT, preferred_element_type=F32)
        mix = jnp.where(causal, mix, 0.0).astype(BF16)
        alive = iota((draft, width), 0) < acc_ref[s]
        end = -rate_x * jnp.sum(jnp.where(alive, dtx, 0.0), axis=0, keepdims=True)
        weight = jnp.where(alive, jnp.exp(jnp.where(alive, end - run, 0.0)) * dtx, 0.0)
        flow = bc_l[0, s].astype(F32).T.astype(BF16)
        early.append((mix, jnp.exp(run), dtx * jnp.exp(-run), weight, jnp.exp(end), flow))

    tile = min(512, span)

    def piece_of(ch):
        return pl.ds(ch * span, span)

    def mix_tokens(s):
        x = xz_l[s, 0].astype(F32)
        z = xz_l[s, 1].astype(F32)
        mix, grown, shrunk = early[s][:3]
        inside = dot(mix, (x * shrunk).astype(BF16))
        y = grown * (inside + dot(bc_l[1, s], st_l[s])) + skip_x * x
        gated = y * z / (1.0 + jnp.exp(-z))
        return x, gated

    def spread(s, gated):
        sums = jnp.sum(gated * gated, axis=1, keepdims=True)
        ss_l[s, me] = jnp.sum(jnp.where(level_eye, sums, 0.0), axis=0, keepdims=True)
        for o in range(1, group):
            peer = lax.rem(me + o, group)
            remote(
                7, ss_l.at[s, me], ss_l.at[s, me], ss_recv.at[s],
                {"head": peer // n_tok, "tok": lax.rem(peer, n_tok)},
            )

    def project(s, normed):
        for ch in range(chunks):
            for start in range(ch * span, (ch + 1) * span, tile):
                val = dot(normed, w_v[:, start : start + tile])
                for g in range(half):
                    for p in range(2):
                        at = (g * 2 + p) * per
                        hold = lax.rem(p + head + line + g // lines + g % lines, 2)
                        part[s, hold, g // lines, g % lines, :, start : start + tile] = val[
                            at : at + per
                        ].astype(BF16)
            remote(
                8, part.at[s, 1 - side, :, :, :, piece_of(ch)],
                pair_l.at[s, :, :, :, piece_of(ch)], pair_recv.at[s, ch], partner,
            )

    def commit(s, x):
        weight, decay, flow = early[s][3:]
        new = decay * st_l[s].astype(F32) + dot(flow, (x * weight).astype(BF16))
        cm_s[s] = new.astype(BF16)
        for o in range(1, n_tok):
            to = lax.rem(tok + o, n_tok)
            remote(
                9, cm_s.at[s, place(to, cols), :], cm_l.at[s, :, place(tok, width)],
                got.at[2], {"tok": to},
            )
        cm_l[s, :, place(tok, width)] = cm_s[s, place(tok, cols), :]

    def above(o):
        return {"head": lax.rem(head + o, n_head), "tok": line * 2 + lax.rem(side + o, 2)}

    def line_first(ch):
        return ch % 2 == 0

    def forward(s, ch):
        piece = piece_of(ch)
        take(pair_recv.at[s, ch], pair_l.at[s, :, :, :, piece])
        red[s, :, :, :, piece] = (
            part[s, side, :, :, :, piece].astype(F32) + pair_l[s, :, :, :, piece].astype(F32)
        ).astype(BF16)
        if line_first(ch):
            for o in range(1, lines):
                to = lax.rem(line + o, lines)
                remote(
                    10, red.at[s, :, to, :, piece], one_a.at[s, o, :, :, piece],
                    one_recv.at[s, ch, o - 1], {"tok": across(o)},
                )
        else:
            for o in range(1, n_head):
                to = lax.rem(head + o, n_head)
                remote(
                    11, red.at[s, to, :, :, piece], one_b.at[s, o, :, :, piece],
                    one_recv.at[s, ch, o - 1], above(o),
                )

    def factor(s, source, base):
        total = jnp.zeros((1, draft), F32)
        for t in range(n_tok):
            total = total + ss_l[s, source * n_tok + t]
        here = iota((per, draft), 1) == base * per + iota((per, draft), 0)
        column = jnp.sum(jnp.where(here, total, 0.0), axis=1, keepdims=True)
        return lax.rsqrt(column / (width * n_tok) + EPSILON)

    def second(s, ch, factors):
        piece = piece_of(ch)
        if line_first(ch):
            for o in range(1, lines):
                take(one_recv.at[s, ch, o - 1], one_a.at[s, o, :, :, piece])
            total = red[s, :, line, :, piece].astype(F32)
            for o in range(1, lines):
                total = total + one_a[s, o, :, :, piece].astype(F32)
            mid_a[s, :, :, piece] = total.astype(BF16)
            for o in range(1, n_head):
                to = lax.rem(head + o, n_head)
                remote(
                    12, mid_a.at[s, to, :, piece], two_a.at[s, o, :, piece],
                    two_recv.at[s, ch, o - 1], above(o),
                )
        else:
            for o in range(1, n_head):
                take(one_recv.at[s, ch, o - 1], one_b.at[s, o, :, :, piece])
            for l in range(lines):
                total = red[s, head, l, :, piece].astype(F32) * factors[0][l]
                for o in range(1, n_head):
                    total = total + one_b[s, o, l, :, piece].astype(F32) * factors[o][l]
                mid_b[s, l, :, piece] = total.astype(BF16)
            for o in range(1, lines):
                to = lax.rem(line + o, lines)
                remote(
                    13, mid_b.at[s, to, :, piece], two_b.at[s, o, :, piece],
                    two_recv.at[s, ch, o - 1], {"tok": across(o)},
                )

    def final(s, ch, factors):
        piece = piece_of(ch)
        if line_first(ch):
            for o in range(1, n_head):
                take(two_recv.at[s, ch, o - 1], two_a.at[s, o, :, piece])
            total = mid_a[s, head, :, piece].astype(F32) * factors[0]
            for o in range(1, n_head):
                total = total + two_a[s, o, :, piece].astype(F32) * factors[o]
        else:
            for o in range(1, lines):
                take(two_recv.at[s, ch, o - 1], two_b.at[s, o, :, piece])
            total = mid_b[s, line, :, piece].astype(F32)
            for o in range(1, lines):
                total = total + two_b[s, o, :, piece].astype(F32)
        return total

    for s in range(seqs):
        take(st_recv.at[s], st_l.at[s, pl.ds(0, (n_tok - 1) * cols), :])
        take(xz_recv.at[s], xz_l.at[s, :, pl.ds(0, (n_tok - 1) * block), :])
        x, gated = mix_tokens(s)
        project(s, (gated * gain).astype(BF16))
        spread(s, gated)
        commit(s, x)
        for ch in range(chunks):
            forward(s, ch)

    take(got.at[0], n_l.at[pl.ds(0, n_tok - 1)])
    take(got.at[1], stat_l.at[pl.ds(0, n_tok - 1)])
    lanes = iota((m_own, m_pair), 1)
    r = iota((m_own, m_pair), 0)
    want = None
    for h in range(per_kv):
        t = r - h * block
        hit = (t >= 0) & (t < block) & (lanes == h * pair + side * block + t)
        want = hit if want is None else want | hit
    for s in range(seqs):
        levels = [
            jnp.sum(jnp.where(want, stat_l[t, s : s + 1, :], 0.0), axis=1, keepdims=True)
            for t in range(n_tok)
        ]
        top = functools.reduce(jnp.maximum, levels)
        weights = [jnp.exp(level - top) for level in levels]
        den = functools.reduce(jnp.add, weights)
        acc = jnp.zeros((m_own, att), F32)
        for t in range(n_tok):
            acc = acc + weights[t] * n_l[t, s].astype(F32)
        acc = (acc / den).astype(BF16)
        for h in range(per_kv):
            ctx_ref[s, :, h * att : (h + 1) * att] = acc[h * block : (h + 1) * block]

    narrow = []
    for s in range(seqs):
        take(ss_recv.at[s], ss_l.at[s, pl.ds(0, group - 1)])
        sources = [lax.rem(head - o + n_head, n_head) for o in range(n_head)]
        places = [(head * lines + l) * 2 + lax.rem(side + line + l, 2) for l in range(lines)]
        wide = [[factor(s, source, at) for at in places] for source in sources]
        narrow.append([factor(s, source, me) for source in sources])
        for ch in range(chunks):
            second(s, ch, wide)

    take(got.at[2], cm_l.at[:, :, pl.ds(0, (n_tok - 1) * width)])
    for s in range(seqs):
        for h in range(heads):
            com_ref[s, h] = cm_l[s, :, h * size : (h + 1) * size]

    at, of = iota((per * seqs, per * seqs), 0), iota((per * seqs, per * seqs), 1)
    weave = jnp.zeros((per * seqs, per * seqs), F32)
    for s in range(seqs):
        weave = jnp.where(at == (of - s * per) * seqs + s, jnp.where((of >= s * per) & (of < (s + 1) * per), 1.0, weave), weave)
    weave = weave.astype(BF16)
    for ch in range(chunks):
        both = jnp.concatenate([final(s, ch, narrow[s]) for s in range(seqs)], axis=0)
        both = dot(weave, both.astype(BF16)).astype(BF16)
        for d in range(per):
            out_ref[d, :, piece_of(ch)] = both[d * seqs : (d + 1) * seqs]

    others = pl.ds(0, n_tok - 1)
    most = pl.ds(0, (n_tok - 1) * block)
    take(sent.at[0], q_l.at[:, most, :])
    take(sent.at[1], bc_l.at[:, :, most, :])
    take(sent.at[2], dt_l.at[:, most, :])
    take(sent.at[3], turn_v.at[:, :, pl.ds(0, (n_tok - 1) * width)])
    take(sent.at[4], xz_v.at[:, :, :, pl.ds(0, (n_tok - 1) * width)])
    take(sent.at[5], n_s.at[others])
    take(sent.at[6], stat_l.at[others])
    take(sent.at[7], ss_l.at[:, pl.ds(0, group - 1)])
    take(sent.at[8], pair_l)
    take(sent.at[9], cm_s.at[:, pl.ds(0, (n_tok - 1) * cols), :])
    partial = pl.ds(0, out_cols // 2)
    take(sent.at[10], one_a.at[:, pl.ds(1, lines - 1), :, :, partial])
    take(sent.at[11], one_b.at[:, pl.ds(1, n_head - 1), :, :, partial])
    take(sent.at[12], two_a.at[:, pl.ds(1, n_head - 1), :, partial])
    take(sent.at[13], two_b.at[:, pl.ds(1, lines - 1), :, partial])


def finish(out_v, ctx_v, com_v, out_ref, ctx_ref, com_ref, sems):
    copies = [
        pltpu.make_async_copy(src, dst, sems.at[i])
        for i, (src, dst) in enumerate(((out_v, out_ref), (com_v, com_ref), (ctx_v, ctx_ref)))
    ]
    for copy in copies:
        copy.start()
    for copy in copies:
        copy.wait()


def body(
    mamba_input, gate_input, in_b, in_c, step_size, decay_rate, skip_weight, norm_gain,
    ssm_state, out_weight, queries, draft_token_keys, draft_values, cached_key_rows,
    cache_values, cache_len, accepted,
):
    n_tok = lax.axis_size("tok")
    n_head = lax.axis_size("head")
    group = n_head * n_tok
    lines = n_tok // 2
    seqs, block, features = mamba_input.shape
    heads = decay_rate.shape[0]
    size = features // heads
    cols = ssm_state.shape[3]
    state = cols * n_tok
    draft = block * n_tok
    width = features // n_tok
    att = draft_token_keys.shape[2]
    per_kv = queries.shape[2] // att
    cache = cached_key_rows.shape[1]
    out_cols = out_weight.shape[1]
    per = draft // group
    chunks = 4
    hops = max(lines, n_head) - 1
    turned = jnp.transpose(ssm_state, (0, 1, 3, 2))
    shapes = (
        (per, seqs, out_cols),
        (seqs, block, per_kv * att),
        (seqs, heads, cols, size),
    )
    operands = (
        mamba_input, gate_input, in_b, in_c, step_size, turned, queries, cached_key_rows,
        cache_values, out_weight, draft_token_keys, draft_values,
        norm_gain.reshape(1, features), decay_rate, skip_weight, cache_len, accepted,
    )
    vmem = pl.BlockSpec(memory_space=pltpu.VMEM)
    held = pl.pallas_call(
        functools.partial(kernel, (n_head, n_tok, seqs, block, heads, chunks)),
        out_shape=[pltpu.VMEM(shape, BF16) for shape in shapes],
        in_specs=[pl.BlockSpec(memory_space=pltpu.HBM)] * len(operands),
        out_specs=[vmem] * 3,
        scratch_shapes=[
            pltpu.VMEM((seqs, 2, block, features), BF16),
            pltpu.VMEM((seqs, 2, draft, width), BF16),
            pltpu.VMEM((2, seqs, draft, state), BF16),
            pltpu.VMEM((seqs, draft, heads), BF16),
            pltpu.VMEM((seqs, heads, cols, size), BF16),
            pltpu.VMEM((seqs, cols, features), BF16),
            pltpu.VMEM((seqs, state, width), BF16),
            pltpu.VMEM((seqs, draft, per_kv * att), BF16),
            pltpu.VMEM((2, seqs, cache, att), BF16),
            pltpu.VMEM((2, seqs, block, att), BF16),
            pltpu.VMEM(out_weight.shape, BF16),
            pltpu.VMEM((1, features), F32),
            pltpu.VMEM((seqs, group, 1, draft), F32),
            pltpu.VMEM((seqs, state, width), BF16),
            pltpu.VMEM((seqs, cols, features), BF16),
            pltpu.VMEM((n_tok, seqs, per_kv * block, att), BF16),
            pltpu.VMEM((n_tok, seqs, per_kv * block, att), BF16),
            pltpu.VMEM((lines, seqs, 2 * per_kv * block), F32),
            pltpu.VMEM((n_tok, seqs, 2 * per_kv * block), F32),
            pltpu.VMEM((seqs, 2, n_head, lines, per, out_cols), BF16),
            pltpu.VMEM((seqs, n_head, lines, per, out_cols), BF16),
            pltpu.VMEM((seqs, n_head, lines, per, out_cols), BF16),
            pltpu.VMEM((seqs, lines, n_head, per, out_cols), BF16),
            pltpu.VMEM((seqs, n_head, lines, per, out_cols), BF16),
            pltpu.VMEM((seqs, n_head, per, out_cols), BF16),
            pltpu.VMEM((seqs, lines, per, out_cols), BF16),
            pltpu.VMEM((seqs, n_head, per, out_cols), BF16),
            pltpu.VMEM((seqs, lines, per, out_cols), BF16),
            pltpu.SMEM(decay_rate.shape, F32),
            pltpu.SMEM(skip_weight.shape, F32),
            pltpu.SMEM(cache_len.shape, jnp.int32),
            pltpu.SMEM(accepted.shape, jnp.int32),
            pltpu.SemaphoreType.DMA((14,)),
            pltpu.SemaphoreType.DMA((n_tok - 1,)),
            pltpu.SemaphoreType.DMA((lines,)),
            pltpu.SemaphoreType.DMA((lines,)),
            pltpu.SemaphoreType.DMA((seqs,)),
            pltpu.SemaphoreType.DMA((seqs,)),
            pltpu.SemaphoreType.DMA((3,)),
            pltpu.SemaphoreType.DMA((seqs,)),
            pltpu.SemaphoreType.DMA((seqs, chunks)),
            pltpu.SemaphoreType.DMA((seqs, chunks, hops)),
            pltpu.SemaphoreType.DMA((seqs, chunks, hops)),
            pltpu.SemaphoreType.DMA((13,)),
        ],
        compiler_params=pltpu.CompilerParams(
            collective_id=0, has_side_effects=True, vmem_limit_bytes=40 * 1024 * 1024
        ),
        name="hybrid",
    )(*[pltpu.with_memory_space_constraint(a, pltpu.HBM) for a in operands])
    out, ctx, com = pl.pallas_call(
        finish,
        out_shape=[jax.ShapeDtypeStruct(shape, BF16) for shape in shapes],
        in_specs=[vmem] * 3,
        out_specs=[pl.BlockSpec(memory_space=pl.ANY)] * 3,
        scratch_shapes=[pltpu.SemaphoreType.DMA((3,))],
        compiler_params=pltpu.CompilerParams(vmem_limit_bytes=4 * 1024 * 1024),
        name="finish",
    )(*[pltpu.with_memory_space_constraint(a, pltpu.VMEM) for a in held])
    return (out, ctx, jnp.transpose(com, (0, 1, 3, 2)))


def solution(mesh):
    in_specs = (
        P("dp", "tok", "head"),
        P("dp", "tok", "head"),
        P("dp", "tok", "head"),
        P("dp", "tok", "head"),
        P("dp", "tok", "head"),
        P("head"),
        P("head"),
        P("head"),
        P("dp", "head", None, "tok"),
        P(("head", "tok"), None),
        P("dp", "tok", "head"),
        P("dp", "tok", "head"),
        P("dp", "tok", "head"),
        P("dp", "tok", "head"),
        P("dp", "tok", "head"),
        P("dp"),
        P("dp"),
    )
    out_specs = (
        P(("head", "tok"), "dp", None),
        P("dp", "tok", "head"),
        P("dp", "head", None, "tok"),
    )
    return jax.shard_map(body, mesh=mesh, in_specs=in_specs, out_specs=out_specs, check_vma=False)
```

```python
import functools
import jax
import jax.numpy as jnp
from jax import lax
from jax.experimental import pallas as pl
from jax.experimental.pallas import tpu as pltpu
from jax.sharding import PartitionSpec as P

EPSILON = 1e-05
MASKED = -1e30
FLOOR = -1e29
MESH = pl.DeviceIdType.MESH
F32 = jnp.float32
BF16 = jnp.bfloat16
NT = (((1,), (1,)), ((), ()))


def dot(a, b):
    return jnp.dot(a, b, preferred_element_type=F32)


def iota(shape, dim):
    return lax.broadcasted_iota(jnp.int32, shape, dim)


PLAN = ("ABAB", "ABAB")
EARLY = (0,)
LATE = 0
WEAVE = 2


def kernel(
    dims,
    x_in, z_in, b_in, c_in, dt_in, st_in, q_in, k_in, v_in, w_in,
    dk_in, dv_in, gain_in, rate_in, skip_in, len_in, acc_in,
    out_ref, ctx_ref, com_ref,
    xz_v, xz_l, bc_l, dt_v, raw_v, turn_v, st_l, q_l, kv_v, new_v, w_v, gain_v,
    ss_l, cm_s, cm_l, n_s, n_l, stat_s, stat_l,
    part, pair_l, red, one_a, one_b, mid_a, mid_b, two_a, two_b,
    heads_ref, seqs_ref,
    sent, q_recv, bc_recv, st_recv, xz_recv, got, ss_recv,
    pair_recv, one_recv, two_recv, local,
):
    n_head, n_tok, seqs, block, heads, plan = dims
    chunks = len(plan[0])
    counts = [row.count("A") for row in plan]
    kinds = [sorted(set(counts)).index(count) for count in counts]
    group = n_head * n_tok
    tok = lax.axis_index("tok")
    head = lax.axis_index("head")
    me = head * n_tok + tok
    draft = block * n_tok
    width = xz_l.shape[3]
    own = heads // n_tok
    size = width // own
    state = st_l.shape[1]
    cols = state // n_tok
    att = kv_v.shape[3]
    per_kv = q_l.shape[2] // att
    cache = kv_v.shape[2]
    per = draft // group
    out_cols = w_v.shape[1]
    span = out_cols // chunks
    half = group // 2
    side = lax.rem(tok, 2)
    line = tok // 2
    lines = n_tok // 2
    slot = head * lines + line

    def place(index, unit):
        return pl.ds(pl.multiple_of(index * unit, unit), unit)

    barrier = pltpu.get_barrier_semaphore()
    for o in range(1, group):
        peer = lax.rem(me + o, group)
        pl.semaphore_signal(
            barrier, inc=1,
            device_id={"head": peer // n_tok, "tok": lax.rem(peer, n_tok)},
            device_id_type=MESH,
        )

    def take(sem, ref):
        pltpu.make_async_copy(ref, ref, sem).wait()

    mine = place(tok, block)
    for sem, src, dst in (
        (0, st_in, raw_v),
        (1, q_in, q_l.at[:, mine, :]),
        (2, b_in, bc_l.at[0, :, mine, :]),
        (2, c_in, bc_l.at[1, :, mine, :]),
        (3, dt_in, dt_v),
        (4, x_in, xz_v.at[:, 0]),
        (4, z_in, xz_v.at[:, 1]),
        (5, dk_in, new_v.at[0]),
        (5, dv_in, new_v.at[1]),
        (6, k_in, kv_v.at[0]),
        (6, v_in, kv_v.at[1]),
        (7, len_in, seqs_ref.at[0]),
        (7, acc_in, seqs_ref.at[1]),
        (8, rate_in, heads_ref.at[0]),
        (8, skip_in, heads_ref.at[1]),
        (9, gain_in, gain_v),
        (10, w_in, w_v),
    ):
        pltpu.make_async_copy(src, dst, local.at[sem]).start()

    take(local.at[0], raw_v)
    for s in range(seqs):
        turn_v[s] = jnp.concatenate(
            [raw_v[s, h].astype(F32) for h in range(heads)], axis=1
        ).astype(BF16)
    st_l[:, place(tok, cols), :] = turn_v[:, :, place(tok, width)]
    take(local.at[1], q_l.at[:, mine, :])
    take(local.at[2], bc_l.at[pl.ds(0, 2), :, mine, :])
    take(local.at[3], dt_v)
    pad = jnp.zeros((seqs, block, state - heads), BF16)
    bc_l[2, :, mine, :] = jnp.concatenate([dt_v[...], pad], axis=2)
    take(local.at[4], xz_v)
    xz_l[:, :, mine, :] = xz_v[:, :, :, place(tok, width)]

    pl.semaphore_wait(barrier, group - 1)

    def remote(kind, src, dst, recv_sem, device):
        pltpu.make_async_remote_copy(
            src_ref=src, dst_ref=dst, send_sem=sent.at[kind], recv_sem=recv_sem,
            device_id=device, device_id_type=MESH,
        ).start()

    flip = tok + 1 - 2 * side
    partner = {"tok": flip}

    def share(at, device, q_sem, sem, only=None):
        span_at = place(at, block)
        for kind, ref, recv in (
            (0, q_l.at[:, span_at, :], q_recv.at[q_sem]),
            (1, bc_l.at[:, :, span_at, :], bc_recv.at[sem]),
        ):
            if only is None or kind in only:
                remote(kind, ref, ref, recv, device)

    def across(o):
        return lax.rem(line + o, lines) * 2 + lax.rem(side + o, 2)

    def origin(o, near):
        return lax.rem(line - o + lines, lines) * 2 + lax.rem(near + o, 2)

    for o in range(1, lines):
        share(tok, {"tok": across(o)}, o, o)
    share(tok, partner, 0, 0)
    for s in range(seqs):
        for o in range(1, n_tok):
            to = lax.rem(tok + o, n_tok)
            remote(
                3, turn_v.at[s, :, place(to, width)], st_l.at[s, place(tok, cols), :],
                st_recv.at[s], {"tok": to},
            )
        for o in range(1, n_tok):
            to = lax.rem(tok + o, n_tok)
            remote(
                4, xz_v.at[s, :, :, place(to, width)], xz_l.at[s, :, mine, :],
                xz_recv.at[s], {"tok": to},
            )

    take(local.at[7], seqs_ref)
    take(local.at[8], heads_ref)
    take(local.at[5], new_v)
    take(local.at[6], kv_v)
    scale = att ** (-0.5)
    m_own = per_kv * block
    eye = iota((m_own, m_own), 0) == iota((m_own, m_own), 1)
    position = tok * cache + iota((1, cache), 1)

    def attend(at, count):
        first, height = at * count, count * block
        inner = iota((height, block), 1) - iota((height, block), 0)
        inner = jnp.concatenate([inner] * per_kv, axis=0)
        r, lanes = (iota((per_kv * height, m_own), d) for d in range(2))
        picks = []
        for c in range(count):
            pick = None
            for h in range(per_kv):
                t = r - (h * count + c) * block
                hit = (t >= 0) & (t < block) & (lanes == h * block + t)
                pick = hit if pick is None else pick | hit
            picks.append(pick)
        for s in range(seqs):
            q = jnp.concatenate(
                [q_l[s, place(at, height), h * att : (h + 1) * att] for h in range(per_kv)], axis=0
            )
            old = lax.dot_general(q, kv_v[0, s], NT, preferred_element_type=F32)
            old = jnp.where(position < seqs_ref[0, s], old, MASKED)
            new = lax.dot_general(q, new_v[0, s], NT, preferred_element_type=F32)
            new = jnp.where(inner <= (first - tok) * block, new, MASKED)
            peak = jnp.maximum(
                jnp.max(old, axis=1, keepdims=True), jnp.max(new, axis=1, keepdims=True)
            )
            peak = jnp.maximum(peak, FLOOR)
            old = jnp.exp((old - peak) * scale)
            new = jnp.exp((new - peak) * scale)
            total = jnp.sum(old, axis=1, keepdims=True) + jnp.sum(new, axis=1, keepdims=True)
            numer = dot(old.astype(BF16), kv_v[1, s]) + dot(new.astype(BF16), new_v[1, s])
            safe = jnp.maximum(total, 1e-30)
            level = jnp.where(total > 0.0, peak * scale + jnp.log(safe), MASKED)
            ctx = (numer / safe).astype(BF16)
            for c in range(count):
                for h in range(per_kv):
                    n_s[first + c, s, h * block : (h + 1) * block] = ctx[
                        (h * count + c) * block : (h * count + c + 1) * block
                    ]
                stat_s[first + c, s] = jnp.sum(
                    jnp.where(picks[c], level, 0.0), axis=0, keepdims=True
                )

    def answer(t):
        remote(5, n_s.at[t], n_l.at[tok], got.at[0], {"tok": t})
        remote(6, stat_s.at[t], stat_l.at[tok], got.at[1], {"tok": t})

    take(q_recv.at[0], q_l.at[:, mine, :])
    attend(line, 2)
    answer(flip)
    n_l[tok] = n_s[tok]
    stat_l[tok] = stat_s[tok]
    for o in range(1, lines):
        take(q_recv.at[o], q_l.at[:, mine, :])
        share(origin(o, side), partner, lines - 1 + o, 0, (0,))
    for o in range(1, lines):
        attend(origin(o, side), 1)
        answer(origin(o, side))
    for o in range(1, lines):
        take(bc_recv.at[o], bc_l.at[:, :, mine, :])
        share(origin(o, side), partner, 0, 0, (1,))
    for o in range(1, lines):
        take(q_recv.at[lines - 1 + o], q_l.at[:, mine, :])
        attend(origin(o, 1 - side), 1)
        answer(origin(o, 1 - side))

    lane = iota((1, width), 1)
    rate_x = jnp.zeros((1, width), F32)
    skip_x = jnp.zeros((1, width), F32)
    for h in range(own):
        inside = (lane >= h * size) & (lane < (h + 1) * size)
        rate_x = jnp.where(inside, heads_ref[0, tok * own + h], rate_x)
        skip_x = jnp.where(inside, heads_ref[1, tok * own + h], skip_x)
    offset = iota((state, width), 1) - (iota((state, width), 0) - tok * own) * size
    pick = ((offset >= 0) & (offset < size)).astype(F32).astype(BF16)
    causal = iota((draft, draft), 0) >= iota((draft, draft), 1)
    lower = causal.astype(F32).astype(BF16)

    level_eye = iota((draft, draft), 0) == iota((draft, draft), 1)
    take(local.at[9], gain_v)
    gain = gain_v[:, place(tok, width)]
    take(local.at[10], w_v)
    take(bc_recv.at[0], bc_l.at[:, :, pl.ds(0, lines * block), :])
    early = {}

    def prepare(s):
        dtx = dot(bc_l[2, s], pick)
        run = -rate_x * dot(lower, dtx.astype(BF16))
        mix = lax.dot_general(bc_l[1, s], bc_l[0, s], NT, preferred_element_type=F32)
        mix = jnp.where(causal, mix, 0.0).astype(BF16)
        alive = iota((draft, width), 0) < seqs_ref[1, s]
        end = -rate_x * jnp.sum(jnp.where(alive, dtx, 0.0), axis=0, keepdims=True)
        weight = jnp.where(alive, jnp.exp(jnp.where(alive, end - run, 0.0)) * dtx, 0.0)
        flow = bc_l[0, s].astype(F32).T.astype(BF16)
        early[s] = (mix, jnp.exp(run), dtx * jnp.exp(-run), weight, jnp.exp(end), flow)

    prepare(0)

    tile = min(512, span)

    def piece_of(ch):
        return pl.ds(ch * span, span)

    def mix_tokens(s):
        x = xz_l[s, 0].astype(F32)
        z = xz_l[s, 1].astype(F32)
        mix, grown, shrunk = early[s][:3]
        inside = dot(mix, (x * shrunk).astype(BF16))
        y = grown * (inside + dot(bc_l[1, s], st_l[s])) + skip_x * x
        gated = y * z / (1.0 + jnp.exp(-z))
        return x, gated

    def spread(s, gated):
        sums = jnp.sum(gated * gated, axis=1, keepdims=True)
        ss_l[s, me] = jnp.sum(jnp.where(level_eye, sums, 0.0), axis=0, keepdims=True)
        for o in range(1, group):
            peer = lax.rem(me + o, group)
            remote(
                7, ss_l.at[s, me], ss_l.at[s, me], ss_recv.at[s],
                {"head": peer // n_tok, "tok": lax.rem(peer, n_tok)},
            )

    def project(s, normed, between):
        for ch in range(chunks):
            for start in range(ch * span, (ch + 1) * span, tile):
                val = dot(normed, w_v[:, start : start + tile])
                for g in range(half):
                    for p in range(2):
                        at = (g * 2 + p) * per
                        hold = lax.rem(p + head + line + g // lines + g % lines, 2)
                        part[s, hold, g // lines, g % lines, :, start : start + tile] = val[
                            at : at + per
                        ].astype(BF16)
            remote(
                8, part.at[s, 1 - side, :, :, :, piece_of(ch)],
                pair_l.at[s, :, :, :, piece_of(ch)], pair_recv.at[s, ch], partner,
            )
            between(ch)

    def commit(s, x):
        weight, decay, flow = early[s][3:]
        new = decay * st_l[s].astype(F32) + dot(flow, (x * weight).astype(BF16))
        cm_s[s] = new.astype(BF16)
        cm_l[s, :, place(tok, width)] = cm_s[s, place(tok, cols), :]

    def hand_out(s):
        for o in range(1, n_tok):
            to = lax.rem(tok + o, n_tok)
            remote(
                9, cm_s.at[s, place(to, cols), :], cm_l.at[s, :, place(tok, width)],
                got.at[2], {"tok": to},
            )

    def above(o):
        return {"head": lax.rem(head + o, n_head), "tok": line * 2 + lax.rem(side + o, 2)}

    def forward(s, ch):
        piece = piece_of(ch)
        take(pair_recv.at[s, ch], pair_l.at[s, :, :, :, piece])
        red[s, :, :, :, piece] = (
            part[s, side, :, :, :, piece].astype(F32) + pair_l[s, :, :, :, piece].astype(F32)
        ).astype(BF16)
        if plan[s][ch] == "A":
            for o in range(1, lines):
                to = lax.rem(line + o, lines)
                remote(
                    10 + 4 * kinds[s], red.at[s, :, to, :, piece], one_a.at[s, o, :, :, piece],
                    one_recv.at[s, ch, o - 1], {"tok": across(o)},
                )
        else:
            for o in range(1, n_head):
                to = lax.rem(head + o, n_head)
                remote(
                    11 + 4 * kinds[s], red.at[s, to, :, :, piece], one_b.at[s, o, :, :, piece],
                    one_recv.at[s, ch, o - 1], above(o),
                )

    def factor(s, source, base):
        total = jnp.zeros((1, draft), F32)
        for t in range(n_tok):
            total = total + ss_l[s, source * n_tok + t]
        here = iota((per, draft), 1) == base * per + iota((per, draft), 0)
        column = jnp.sum(jnp.where(here, total, 0.0), axis=1, keepdims=True)
        return lax.rsqrt(column / (width * n_tok) + EPSILON)

    def second(s, ch, factors):
        piece = piece_of(ch)
        if plan[s][ch] == "A":
            for o in range(1, lines):
                take(one_recv.at[s, ch, o - 1], one_a.at[s, o, :, :, piece])
            total = red[s, :, line, :, piece].astype(F32)
            for o in range(1, lines):
                total = total + one_a[s, o, :, :, piece].astype(F32)
            mid_a[s, :, :, piece] = total.astype(BF16)
            for o in range(1, n_head):
                to = lax.rem(head + o, n_head)
                remote(
                    12 + 4 * kinds[s], mid_a.at[s, to, :, piece], two_a.at[s, o, :, piece],
                    two_recv.at[s, ch, o - 1], above(o),
                )
        else:
            for o in range(1, n_head):
                take(one_recv.at[s, ch, o - 1], one_b.at[s, o, :, :, piece])
            for l in range(lines):
                total = red[s, head, l, :, piece].astype(F32) * factors[0][l]
                for o in range(1, n_head):
                    total = total + one_b[s, o, l, :, piece].astype(F32) * factors[o][l]
                mid_b[s, l, :, piece] = total.astype(BF16)
            for o in range(1, lines):
                to = lax.rem(line + o, lines)
                remote(
                    13 + 4 * kinds[s], mid_b.at[s, to, :, piece], two_b.at[s, o, :, piece],
                    two_recv.at[s, ch, o - 1], {"tok": across(o)},
                )

    def final(s, ch, factors):
        piece = piece_of(ch)
        if plan[s][ch] == "A":
            for o in range(1, n_head):
                take(two_recv.at[s, ch, o - 1], two_a.at[s, o, :, piece])
            total = mid_a[s, head, :, piece].astype(F32) * factors[0]
            for o in range(1, n_head):
                total = total + two_a[s, o, :, piece].astype(F32) * factors[o]
        else:
            for o in range(1, lines):
                take(two_recv.at[s, ch, o - 1], two_b.at[s, o, :, piece])
            total = mid_b[s, line, :, piece].astype(F32)
            for o in range(1, lines):
                total = total + two_b[s, o, :, piece].astype(F32)
        return total

    for s in range(seqs):
        take(st_recv.at[s], st_l.at[s, pl.ds(0, (n_tok - 1) * cols), :])
        take(xz_recv.at[s], xz_l.at[s, :, pl.ds(0, (n_tok - 1) * block), :])
        x, gated = mix_tokens(s)
        def between(ch, s=s):
            if s > 0 and ch + WEAVE < chunks:
                forward(s - 1, ch + WEAVE)

        project(s, (gated * gain).astype(BF16), between)
        spread(s, gated)
        commit(s, x)
        if s in EARLY:
            hand_out(s)
        if s + 1 < seqs:
            prepare(s + 1)
        for ch in range(chunks if s == seqs - 1 else min(WEAVE, chunks)):
            forward(s, ch)

    narrow = []
    for s in range(seqs):
        take(ss_recv.at[s], ss_l.at[s, pl.ds(0, group - 1)])
        sources = [lax.rem(head - o + n_head, n_head) for o in range(n_head)]
        places = [(head * lines + l) * 2 + lax.rem(side + line + l, 2) for l in range(lines)]
        wide = None
        if "B" in plan[s]:
            wide = [[factor(s, source, at) for at in places] for source in sources]
        near = {}
        if "A" in plan[s]:
            near["A"] = [factor(s, source, me) for source in sources]
        narrow.append(near)
        for ch in range(chunks):
            second(s, ch, wide)
        if s == LATE:
            for later in range(seqs):
                if later not in EARLY:
                    hand_out(later)

    take(got.at[0], n_l.at[pl.ds(0, n_tok - 1)])
    take(got.at[1], stat_l.at[pl.ds(0, n_tok - 1)])
    for s in range(seqs):
        levels = [
            jnp.sum(jnp.where(eye, stat_l[t, s], 0.0), axis=1, keepdims=True)
            for t in range(n_tok)
        ]
        top = functools.reduce(jnp.maximum, levels)
        weights = [jnp.exp(level - top) for level in levels]
        den = functools.reduce(jnp.add, weights)
        acc = jnp.zeros((m_own, att), F32)
        for t in range(n_tok):
            acc = acc + weights[t] * n_l[t, s].astype(F32)
        acc = (acc / den).astype(BF16)
        for h in range(per_kv):
            ctx_ref[s, :, h * att : (h + 1) * att] = acc[h * block : (h + 1) * block]

    take(got.at[2], cm_l.at[:, :, pl.ds(0, (n_tok - 1) * width)])
    for s in range(seqs):
        for h in range(heads):
            com_ref[s, h] = cm_l[s, :, h * size : (h + 1) * size]

    at, of = iota((per * seqs, per * seqs), 0), iota((per * seqs, per * seqs), 1)
    weave = jnp.zeros((per * seqs, per * seqs), F32)
    for s in range(seqs):
        weave = jnp.where(at == (of - s * per) * seqs + s, jnp.where((of >= s * per) & (of < (s + 1) * per), 1.0, weave), weave)
    weave = weave.astype(BF16)
    for ch in range(chunks):
        both = jnp.concatenate([final(s, ch, narrow[s].get(plan[s][ch])) for s in range(seqs)], axis=0)
        both = dot(weave, both.astype(BF16)).astype(BF16)
        for d in range(per):
            out_ref[d, :, piece_of(ch)] = both[d * seqs : (d + 1) * seqs]

    others = pl.ds(0, n_tok - 1)
    most = pl.ds(0, (n_tok - 1) * block)
    take(sent.at[0], q_l.at[:, most, :])
    take(sent.at[1], bc_l.at[:, :, most, :])
    take(sent.at[3], turn_v.at[:, :, pl.ds(0, (n_tok - 1) * width)])
    take(sent.at[4], xz_v.at[:, :, :, pl.ds(0, (n_tok - 1) * width)])
    take(sent.at[5], n_s.at[others])
    take(sent.at[6], stat_l.at[others])
    take(sent.at[7], ss_l.at[:, pl.ds(0, group - 1)])
    take(sent.at[8], pair_l)
    take(sent.at[9], cm_s.at[:, pl.ds(0, (n_tok - 1) * cols), :])
    for k, share_of in enumerate(sorted(set(counts))):
        same = pl.ds(counts.index(share_of), counts.count(share_of))
        a, b = pl.ds(0, share_of * span), pl.ds(0, (chunks - share_of) * span)
        if share_of:
            take(sent.at[10 + 4 * k], one_a.at[same, pl.ds(1, lines - 1), :, :, a])
            take(sent.at[12 + 4 * k], two_a.at[same, pl.ds(1, n_head - 1), :, a])
        if share_of < chunks:
            take(sent.at[11 + 4 * k], one_b.at[same, pl.ds(1, n_head - 1), :, :, b])
            take(sent.at[13 + 4 * k], two_b.at[same, pl.ds(1, lines - 1), :, b])


def finish(out_v, ctx_v, com_v, out_ref, ctx_ref, com_ref, sems):
    copies = [
        pltpu.make_async_copy(src, dst, sems.at[i])
        for i, (src, dst) in enumerate(((out_v, out_ref), (com_v, com_ref), (ctx_v, ctx_ref)))
    ]
    for copy in copies:
        copy.start()
    for copy in copies:
        copy.wait()


def body(
    mamba_input, gate_input, in_b, in_c, step_size, decay_rate, skip_weight, norm_gain,
    ssm_state, out_weight, queries, draft_token_keys, draft_values, cached_key_rows,
    cache_values, cache_len, accepted,
):
    n_tok = lax.axis_size("tok")
    n_head = lax.axis_size("head")
    group = n_head * n_tok
    lines = n_tok // 2
    seqs, block, features = mamba_input.shape
    heads = decay_rate.shape[0]
    size = features // heads
    cols = ssm_state.shape[3]
    state = cols * n_tok
    draft = block * n_tok
    width = features // n_tok
    att = draft_token_keys.shape[2]
    per_kv = queries.shape[2] // att
    cache = cached_key_rows.shape[1]
    out_cols = out_weight.shape[1]
    per = draft // group
    plan = [PLAN[min(s, len(PLAN) - 1)] for s in range(seqs)]
    chunks = len(plan[0])
    hops = max(lines, n_head) - 1
    turned = jnp.transpose(ssm_state, (0, 1, 3, 2))
    shapes = (
        (per, seqs, out_cols),
        (seqs, block, per_kv * att),
        (seqs, heads, cols, size),
    )
    operands = (
        mamba_input, gate_input, in_b, in_c, step_size, turned, queries, cached_key_rows,
        cache_values, out_weight, draft_token_keys, draft_values,
        norm_gain.reshape(1, features), decay_rate, skip_weight, cache_len, accepted,
    )
    vmem = pl.BlockSpec(memory_space=pltpu.VMEM)
    held = pl.pallas_call(
        functools.partial(kernel, (n_head, n_tok, seqs, block, heads, plan)),
        out_shape=[pltpu.VMEM(shape, BF16) for shape in shapes],
        in_specs=[pl.BlockSpec(memory_space=pltpu.HBM)] * len(operands),
        out_specs=[vmem] * 3,
        scratch_shapes=[
            pltpu.VMEM((seqs, 2, block, features), BF16),
            pltpu.VMEM((seqs, 2, draft, width), BF16),
            pltpu.VMEM((3, seqs, draft, state), BF16),
            pltpu.VMEM((seqs, block, heads), BF16),
            pltpu.VMEM((seqs, heads, cols, size), BF16),
            pltpu.VMEM((seqs, cols, features), BF16),
            pltpu.VMEM((seqs, state, width), BF16),
            pltpu.VMEM((seqs, draft, per_kv * att), BF16),
            pltpu.VMEM((2, seqs, cache, att), BF16),
            pltpu.VMEM((2, seqs, block, att), BF16),
            pltpu.VMEM(out_weight.shape, BF16),
            pltpu.VMEM((1, features), F32),
            pltpu.VMEM((seqs, group, 1, draft), F32),
            pltpu.VMEM((seqs, state, width), BF16),
            pltpu.VMEM((seqs, cols, features), BF16),
            pltpu.VMEM((n_tok, seqs, per_kv * block, att), BF16),
            pltpu.VMEM((n_tok, seqs, per_kv * block, att), BF16),
            pltpu.VMEM((n_tok, seqs, 1, per_kv * block), F32),
            pltpu.VMEM((n_tok, seqs, 1, per_kv * block), F32),
            pltpu.VMEM((seqs, 2, n_head, lines, per, out_cols), BF16),
            pltpu.VMEM((seqs, n_head, lines, per, out_cols), BF16),
            pltpu.VMEM((seqs, n_head, lines, per, out_cols), BF16),
            pltpu.VMEM((seqs, lines, n_head, per, out_cols), BF16),
            pltpu.VMEM((seqs, n_head, lines, per, out_cols), BF16),
            pltpu.VMEM((seqs, n_head, per, out_cols), BF16),
            pltpu.VMEM((seqs, lines, per, out_cols), BF16),
            pltpu.VMEM((seqs, n_head, per, out_cols), BF16),
            pltpu.VMEM((seqs, lines, per, out_cols), BF16),
            pltpu.SMEM((2,) + decay_rate.shape, F32),
            pltpu.SMEM((2,) + cache_len.shape, jnp.int32),
            pltpu.SemaphoreType.DMA((10 + 4 * len({row.count("A") for row in plan}),)),
            pltpu.SemaphoreType.DMA((n_tok - 1,)),
            pltpu.SemaphoreType.DMA((lines,)),
            pltpu.SemaphoreType.DMA((seqs,)),
            pltpu.SemaphoreType.DMA((seqs,)),
            pltpu.SemaphoreType.DMA((3,)),
            pltpu.SemaphoreType.DMA((seqs,)),
            pltpu.SemaphoreType.DMA((seqs, chunks)),
            pltpu.SemaphoreType.DMA((seqs, chunks, hops)),
            pltpu.SemaphoreType.DMA((seqs, chunks, hops)),
            pltpu.SemaphoreType.DMA((11,)),
        ],
        compiler_params=pltpu.CompilerParams(
            collective_id=0, has_side_effects=True, vmem_limit_bytes=40 * 1024 * 1024
        ),
        name="hybrid",
    )(*[pltpu.with_memory_space_constraint(a, pltpu.HBM) for a in operands])
    out, ctx, com = pl.pallas_call(
        finish,
        out_shape=[jax.ShapeDtypeStruct(shape, BF16) for shape in shapes],
        in_specs=[vmem] * 3,
        out_specs=[pl.BlockSpec(memory_space=pl.ANY)] * 3,
        scratch_shapes=[pltpu.SemaphoreType.DMA((3,))],
        compiler_params=pltpu.CompilerParams(vmem_limit_bytes=4 * 1024 * 1024),
        name="finish",
    )(*[pltpu.with_memory_space_constraint(a, pltpu.VMEM) for a in held])
    return (out, ctx, jnp.transpose(com, (0, 1, 3, 2)))


def solution(mesh):
    in_specs = (
        P("dp", "tok", "head"),
        P("dp", "tok", "head"),
        P("dp", "tok", "head"),
        P("dp", "tok", "head"),
        P("dp", "tok", "head"),
        P("head"),
        P("head"),
        P("head"),
        P("dp", "head", None, "tok"),
        P(("head", "tok"), None),
        P("dp", "tok", "head"),
        P("dp", "tok", "head"),
        P("dp", "tok", "head"),
        P("dp", "tok", "head"),
        P("dp", "tok", "head"),
        P("dp"),
        P("dp"),
    )
    out_specs = (
        P(("head", "tok"), "dp", None),
        P("dp", "tok", "head"),
        P("dp", "head", None, "tok"),
    )
    return jax.shard_map(body, mesh=mesh, in_specs=in_specs, out_specs=out_specs, check_vma=False)
```

```python
import functools
import jax
import jax.numpy as jnp
from jax import lax
from jax.experimental import pallas as pl
from jax.experimental.pallas import tpu as pltpu
from jax.sharding import PartitionSpec as P

EPSILON = 1e-05
MASKED = -1e30
FLOOR = -1e29
MESH = pl.DeviceIdType.MESH
F32 = jnp.float32
BF16 = jnp.bfloat16
NT = (((1,), (1,)), ((), ()))


def dot(a, b):
    return jnp.dot(a, b, preferred_element_type=F32)


def iota(shape, dim):
    return lax.broadcasted_iota(jnp.int32, shape, dim)


PLAN = ("ABAB", "ABAB")
EARLY = (0,)
LATE = 0
WEAVE = 2
FIRST = 0
POWER = False
LOG2E = 1.4426950408889634


def kernel(
    dims,
    x_in, z_in, b_in, c_in, dt_in, st_in, q_in, k_in, v_in, w_in,
    dk_in, dv_in, gain_in, rate_in, skip_in, len_in, acc_in,
    out_ref, ctx_ref, com_ref,
    xz_v, xz_l, bc_l, dt_v, raw_v, turn_v, st_l, q_l, kv_v, new_v, w_v, gain_v,
    ss_l, cm_s, cm_l, n_s, n_l, stat_s, stat_l,
    part, pair_l, red, one_a, one_b, mid_a, mid_b, two_a, two_b,
    heads_ref, seqs_ref,
    sent, q_recv, bc_recv, st_recv, xz_recv, got, ss_recv,
    pair_recv, one_recv, two_recv, local,
):
    n_head, n_tok, seqs, block, heads, plan = dims
    chunks = len(plan[0])
    counts = [row.count("A") for row in plan]
    kinds = [sorted(set(counts)).index(count) for count in counts]
    group = n_head * n_tok
    tok = lax.axis_index("tok")
    head = lax.axis_index("head")
    me = head * n_tok + tok
    draft = block * n_tok
    width = xz_l.shape[3]
    own = heads // n_tok
    size = width // own
    state = st_l.shape[1]
    cols = state // n_tok
    att = kv_v.shape[3]
    per_kv = q_l.shape[2] // att
    cache = kv_v.shape[2]
    per = draft // group
    out_cols = w_v.shape[1]
    span = out_cols // chunks
    half = group // 2
    side = lax.rem(tok, 2)
    line = tok // 2
    lines = n_tok // 2
    slot = head * lines + line

    def place(index, unit):
        return pl.ds(pl.multiple_of(index * unit, unit), unit)

    barrier = pltpu.get_barrier_semaphore()
    for o in range(1, group):
        peer = lax.rem(me + o, group)
        pl.semaphore_signal(
            barrier, inc=1,
            device_id={"head": peer // n_tok, "tok": lax.rem(peer, n_tok)},
            device_id_type=MESH,
        )

    def take(sem, ref):
        pltpu.make_async_copy(ref, ref, sem).wait()

    mine = place(tok, block)
    for sem, src, dst in (
        (0, st_in, raw_v),
        (1, q_in, q_l.at[:, mine, :]),
        (2, b_in, bc_l.at[0, :, mine, :]),
        (2, c_in, bc_l.at[1, :, mine, :]),
        (3, dt_in, dt_v),
        (4, x_in, xz_v.at[:, 0]),
        (4, z_in, xz_v.at[:, 1]),
        (5, dk_in, new_v.at[0]),
        (5, dv_in, new_v.at[1]),
        (6, k_in, kv_v.at[0]),
        (6, v_in, kv_v.at[1]),
        (7, len_in, seqs_ref.at[0]),
        (7, acc_in, seqs_ref.at[1]),
        (8, rate_in, heads_ref.at[0]),
        (8, skip_in, heads_ref.at[1]),
        (9, gain_in, gain_v),
        (10, w_in, w_v),
    ):
        pltpu.make_async_copy(src, dst, local.at[sem]).start()

    take(local.at[0], raw_v)
    for s in range(seqs):
        turn_v[s] = jnp.concatenate(
            [raw_v[s, h].astype(F32) for h in range(heads)], axis=1
        ).astype(BF16)
    st_l[:, place(tok, cols), :] = turn_v[:, :, place(tok, width)]
    take(local.at[1], q_l.at[:, mine, :])
    take(local.at[2], bc_l.at[pl.ds(0, 2), :, mine, :])
    take(local.at[3], dt_v)
    pad = jnp.zeros((seqs, block, state - heads), BF16)
    bc_l[2, :, mine, :] = jnp.concatenate([dt_v[...], pad], axis=2)
    take(local.at[4], xz_v)
    xz_l[:, :, mine, :] = xz_v[:, :, :, place(tok, width)]

    pl.semaphore_wait(barrier, group - 1)

    def remote(kind, src, dst, recv_sem, device):
        pltpu.make_async_remote_copy(
            src_ref=src, dst_ref=dst, send_sem=sent.at[kind], recv_sem=recv_sem,
            device_id=device, device_id_type=MESH,
        ).start()

    flip = tok + 1 - 2 * side
    partner = {"tok": flip}

    def share(at, device, q_sem, sem, only=None):
        span_at = place(at, block)
        for kind, ref, recv in (
            (0, q_l.at[:, span_at, :], q_recv.at[q_sem]),
            (1, bc_l.at[:, :, span_at, :], bc_recv.at[sem]),
        ):
            if only is None or kind in only:
                remote(kind, ref, ref, recv, device)

    def across(o):
        return lax.rem(line + o, lines) * 2 + lax.rem(side + o, 2)

    def origin(o, near):
        return lax.rem(line - o + lines, lines) * 2 + lax.rem(near + o, 2)

    for o in range(1, lines):
        share(tok, {"tok": across(o)}, o, o)
    share(tok, partner, 0, 0)
    for s in range(seqs):
        for o in range(1, n_tok):
            to = lax.rem(tok + o, n_tok)
            remote(
                3, turn_v.at[s, :, place(to, width)], st_l.at[s, place(tok, cols), :],
                st_recv.at[s], {"tok": to},
            )
        for o in range(1, n_tok):
            to = lax.rem(tok + o, n_tok)
            remote(
                4, xz_v.at[s, :, :, place(to, width)], xz_l.at[s, :, mine, :],
                xz_recv.at[s], {"tok": to},
            )

    take(local.at[7], seqs_ref)
    take(local.at[8], heads_ref)
    take(local.at[5], new_v)
    take(local.at[6], kv_v)
    scale = att ** (-0.5)
    m_own = per_kv * block
    eye = iota((m_own, m_own), 0) == iota((m_own, m_own), 1)
    position = tok * cache + iota((1, cache), 1)

    def attend(at, count):
        first, height = at * count, count * block
        inner = iota((height, block), 1) - iota((height, block), 0)
        inner = jnp.concatenate([inner] * per_kv, axis=0)
        r, lanes = (iota((per_kv * height, m_own), d) for d in range(2))
        picks = []
        for c in range(count):
            pick = None
            for h in range(per_kv):
                t = r - (h * count + c) * block
                hit = (t >= 0) & (t < block) & (lanes == h * block + t)
                pick = hit if pick is None else pick | hit
            picks.append(pick)
        each = range(seqs)
        q = [
            jnp.concatenate(
                [q_l[s, place(at, height), h * att : (h + 1) * att] for h in range(per_kv)], axis=0
            )
            for s in each
        ]
        old = [lax.dot_general(q[s], kv_v[0, s], NT, preferred_element_type=F32) for s in each]
        new = [lax.dot_general(q[s], new_v[0, s], NT, preferred_element_type=F32) for s in each]
        old = [jnp.where(position < seqs_ref[0, s], old[s], MASKED) for s in each]
        new = [jnp.where(inner <= (first - tok) * block, new[s], MASKED) for s in each]
        peak = [
            jnp.maximum(
                jnp.max(old[s], axis=1, keepdims=True), jnp.max(new[s], axis=1, keepdims=True)
            )
            for s in each
        ]
        peak = [jnp.maximum(peak[s], FLOOR) for s in each]
        if POWER:
            lift = [peak[s] * (scale * LOG2E) for s in each]
            old = [jnp.exp2(old[s] * (scale * LOG2E) - lift[s]) for s in each]
            new = [jnp.exp2(new[s] * (scale * LOG2E) - lift[s]) for s in each]
        else:
            old = [jnp.exp((old[s] - peak[s]) * scale) for s in each]
            new = [jnp.exp((new[s] - peak[s]) * scale) for s in each]
        numer = [dot(old[s].astype(BF16), kv_v[1, s]) for s in each]
        numer = [numer[s] + dot(new[s].astype(BF16), new_v[1, s]) for s in each]
        total = [
            jnp.sum(old[s], axis=1, keepdims=True) + jnp.sum(new[s], axis=1, keepdims=True)
            for s in each
        ]
        for s in each:
            safe = jnp.maximum(total[s], 1e-30)
            level = jnp.where(total[s] > 0.0, peak[s] * scale + jnp.log(safe), MASKED)
            ctx = (numer[s] / safe).astype(BF16)
            for c in range(count):
                for h in range(per_kv):
                    n_s[first + c, s, h * block : (h + 1) * block] = ctx[
                        (h * count + c) * block : (h * count + c + 1) * block
                    ]
                stat_s[first + c, s] = jnp.sum(
                    jnp.where(picks[c], level, 0.0), axis=0, keepdims=True
                )

    def answer(t):
        remote(5, n_s.at[t], n_l.at[tok], got.at[0], {"tok": t})
        remote(6, stat_s.at[t], stat_l.at[tok], got.at[1], {"tok": t})

    take(q_recv.at[0], q_l.at[:, mine, :])
    attend(line, 2)
    answer(flip)
    n_l[tok] = n_s[tok]
    stat_l[tok] = stat_s[tok]
    for o in range(1, lines):
        take(q_recv.at[o], q_l.at[:, mine, :])
        share(origin(o, side), partner, lines - 1 + o, 0, (0,))
    for o in range(1, lines):
        attend(origin(o, side), 1)
        answer(origin(o, side))
    for o in range(1, lines):
        take(bc_recv.at[o], bc_l.at[:, :, mine, :])
        share(origin(o, side), partner, 0, 0, (1,))
    for o in range(1, lines):
        take(q_recv.at[lines - 1 + o], q_l.at[:, mine, :])
        attend(origin(o, 1 - side), 1)
        answer(origin(o, 1 - side))

    lane = iota((1, width), 1)
    rate_x = jnp.zeros((1, width), F32)
    skip_x = jnp.zeros((1, width), F32)
    for h in range(own):
        inside = (lane >= h * size) & (lane < (h + 1) * size)
        rate_x = jnp.where(inside, heads_ref[0, tok * own + h], rate_x)
        skip_x = jnp.where(inside, heads_ref[1, tok * own + h], skip_x)
    offset = iota((state, width), 1) - (iota((state, width), 0) - tok * own) * size
    pick = ((offset >= 0) & (offset < size)).astype(F32).astype(BF16)
    causal = iota((draft, draft), 0) >= iota((draft, draft), 1)
    lower = causal.astype(F32).astype(BF16)

    level_eye = iota((draft, draft), 0) == iota((draft, draft), 1)
    take(local.at[9], gain_v)
    gain = gain_v[:, place(tok, width)]
    take(local.at[10], w_v)
    take(bc_recv.at[0], bc_l.at[:, :, pl.ds(0, lines * block), :])
    early = {}

    def prepare(s):
        dtx = dot(bc_l[2, s], pick)
        run = -rate_x * dot(lower, dtx.astype(BF16))
        mix = lax.dot_general(bc_l[1, s], bc_l[0, s], NT, preferred_element_type=F32)
        mix = jnp.where(causal, mix, 0.0).astype(BF16)
        alive = iota((draft, width), 0) < seqs_ref[1, s]
        end = -rate_x * jnp.sum(jnp.where(alive, dtx, 0.0), axis=0, keepdims=True)
        weight = jnp.where(alive, jnp.exp(jnp.where(alive, end - run, 0.0)) * dtx, 0.0)
        flow = bc_l[0, s].astype(F32).T.astype(BF16)
        early[s] = (mix, jnp.exp(run), dtx * jnp.exp(-run), weight, jnp.exp(end), flow)

    prepare(0)

    tile = min(512, span)

    def piece_of(ch):
        return pl.ds(ch * span, span)

    def mix_tokens(s):
        x = xz_l[s, 0].astype(F32)
        z = xz_l[s, 1].astype(F32)
        mix, grown, shrunk = early[s][:3]
        inside = dot(mix, (x * shrunk).astype(BF16))
        y = grown * (inside + dot(bc_l[1, s], st_l[s])) + skip_x * x
        gated = y * z / (1.0 + jnp.exp(-z))
        return gated

    def spread(s, gated):
        sums = jnp.sum(gated * gated, axis=1, keepdims=True)
        ss_l[s, me] = jnp.sum(jnp.where(level_eye, sums, 0.0), axis=0, keepdims=True)
        for o in range(1, group):
            peer = lax.rem(me + o, group)
            remote(
                7, ss_l.at[s, me], ss_l.at[s, me], ss_recv.at[s],
                {"head": peer // n_tok, "tok": lax.rem(peer, n_tok)},
            )

    def project(s, normed, between):
        for ch in range(chunks):
            for start in range(ch * span, (ch + 1) * span, tile):
                val = dot(normed, w_v[:, start : start + tile])
                for g in range(half):
                    for p in range(2):
                        at = (g * 2 + p) * per
                        hold = lax.rem(p + head + line + g // lines + g % lines, 2)
                        part[s, hold, g // lines, g % lines, :, start : start + tile] = val[
                            at : at + per
                        ].astype(BF16)
            remote(
                8, part.at[s, 1 - side, :, :, :, piece_of(ch)],
                pair_l.at[s, :, :, :, piece_of(ch)], pair_recv.at[s, ch], partner,
            )
            between(ch)

    def commit(s):
        x = xz_l[s, 0].astype(F32)
        weight, decay, flow = early[s][3:]
        new = decay * st_l[s].astype(F32) + dot(flow, (x * weight).astype(BF16))
        cm_s[s] = new.astype(BF16)
        cm_l[s, :, place(tok, width)] = cm_s[s, place(tok, cols), :]

    def hand_out(s):
        for o in range(1, n_tok):
            to = lax.rem(tok + o, n_tok)
            remote(
                9, cm_s.at[s, place(to, cols), :], cm_l.at[s, :, place(tok, width)],
                got.at[2], {"tok": to},
            )

    def above(o):
        return {"head": lax.rem(head + o, n_head), "tok": line * 2 + lax.rem(side + o, 2)}

    def forward(s, ch):
        piece = piece_of(ch)
        take(pair_recv.at[s, ch], pair_l.at[s, :, :, :, piece])
        red[s, :, :, :, piece] = (
            part[s, side, :, :, :, piece].astype(F32) + pair_l[s, :, :, :, piece].astype(F32)
        ).astype(BF16)
        if plan[s][ch] == "A":
            for o in range(1, lines):
                to = lax.rem(line + o, lines)
                remote(
                    10 + 4 * kinds[s], red.at[s, :, to, :, piece], one_a.at[s, o, :, :, piece],
                    one_recv.at[s, ch, o - 1], {"tok": across(o)},
                )
        else:
            for o in range(1, n_head):
                to = lax.rem(head + o, n_head)
                remote(
                    11 + 4 * kinds[s], red.at[s, to, :, :, piece], one_b.at[s, o, :, :, piece],
                    one_recv.at[s, ch, o - 1], above(o),
                )

    def factor(s, source, base):
        total = jnp.zeros((1, draft), F32)
        for t in range(n_tok):
            total = total + ss_l[s, source * n_tok + t]
        here = iota((per, draft), 1) == base * per + iota((per, draft), 0)
        column = jnp.sum(jnp.where(here, total, 0.0), axis=1, keepdims=True)
        return lax.rsqrt(column / (width * n_tok) + EPSILON)

    def second(s, ch, factors):
        piece = piece_of(ch)
        if plan[s][ch] == "A":
            for o in range(1, lines):
                take(one_recv.at[s, ch, o - 1], one_a.at[s, o, :, :, piece])
            total = red[s, :, line, :, piece].astype(F32)
            for o in range(1, lines):
                total = total + one_a[s, o, :, :, piece].astype(F32)
            mid_a[s, :, :, piece] = total.astype(BF16)
            for o in range(1, n_head):
                to = lax.rem(head + o, n_head)
                remote(
                    12 + 4 * kinds[s], mid_a.at[s, to, :, piece], two_a.at[s, o, :, piece],
                    two_recv.at[s, ch, o - 1], above(o),
                )
        else:
            for o in range(1, n_head):
                take(one_recv.at[s, ch, o - 1], one_b.at[s, o, :, :, piece])
            for l in range(lines):
                total = red[s, head, l, :, piece].astype(F32) * factors[0][l]
                for o in range(1, n_head):
                    total = total + one_b[s, o, l, :, piece].astype(F32) * factors[o][l]
                mid_b[s, l, :, piece] = total.astype(BF16)
            for o in range(1, lines):
                to = lax.rem(line + o, lines)
                remote(
                    13 + 4 * kinds[s], mid_b.at[s, to, :, piece], two_b.at[s, o, :, piece],
                    two_recv.at[s, ch, o - 1], {"tok": across(o)},
                )

    def final(s, ch, factors):
        piece = piece_of(ch)
        if plan[s][ch] == "A":
            for o in range(1, n_head):
                take(two_recv.at[s, ch, o - 1], two_a.at[s, o, :, piece])
            total = mid_a[s, head, :, piece].astype(F32) * factors[0]
            for o in range(1, n_head):
                total = total + two_a[s, o, :, piece].astype(F32) * factors[o]
        else:
            for o in range(1, lines):
                take(two_recv.at[s, ch, o - 1], two_b.at[s, o, :, piece])
            total = mid_b[s, line, :, piece].astype(F32)
            for o in range(1, lines):
                total = total + two_b[s, o, :, piece].astype(F32)
        return total

    for s in range(seqs):
        take(st_recv.at[s], st_l.at[s, pl.ds(0, (n_tok - 1) * cols), :])
        take(xz_recv.at[s], xz_l.at[s, :, pl.ds(0, (n_tok - 1) * block), :])
        if FIRST == 0 and s in EARLY:
            commit(s)
            hand_out(s)
        gated = mix_tokens(s)

        def between(ch, s=s):
            if s > 0 and ch + WEAVE < chunks:
                forward(s - 1, ch + WEAVE)

        project(s, (gated * gain).astype(BF16), between)
        spread(s, gated)
        if s not in EARLY or FIRST > 0:
            commit(s)
            if s in EARLY and FIRST == 1:
                hand_out(s)
        if s + 1 < seqs:
            prepare(s + 1)
        for ch in range(chunks if s == seqs - 1 else min(WEAVE, chunks)):
            forward(s, ch)
        if FIRST == 3 and s in EARLY:
            hand_out(s)
    for s in range(seqs):
        if FIRST == 2 and s in EARLY:
            hand_out(s)

    narrow = []
    for s in range(seqs):
        take(ss_recv.at[s], ss_l.at[s, pl.ds(0, group - 1)])
        sources = [lax.rem(head - o + n_head, n_head) for o in range(n_head)]
        places = [(head * lines + l) * 2 + lax.rem(side + line + l, 2) for l in range(lines)]
        wide = None
        if "B" in plan[s]:
            wide = [[factor(s, source, at) for at in places] for source in sources]
        near = {}
        if "A" in plan[s]:
            near["A"] = [factor(s, source, me) for source in sources]
        narrow.append(near)
        for ch in range(chunks):
            second(s, ch, wide)
        if s == LATE:
            for later in range(seqs):
                if later not in EARLY:
                    hand_out(later)

    take(got.at[0], n_l.at[pl.ds(0, n_tok - 1)])
    take(got.at[1], stat_l.at[pl.ds(0, n_tok - 1)])
    for s in range(seqs):
        levels = [
            jnp.sum(jnp.where(eye, stat_l[t, s], 0.0), axis=1, keepdims=True)
            for t in range(n_tok)
        ]
        top = functools.reduce(jnp.maximum, levels)
        weights = [jnp.exp(level - top) for level in levels]
        den = functools.reduce(jnp.add, weights)
        acc = jnp.zeros((m_own, att), F32)
        for t in range(n_tok):
            acc = acc + weights[t] * n_l[t, s].astype(F32)
        acc = (acc / den).astype(BF16)
        for h in range(per_kv):
            ctx_ref[s, :, h * att : (h + 1) * att] = acc[h * block : (h + 1) * block]

    take(got.at[2], cm_l.at[:, :, pl.ds(0, (n_tok - 1) * width)])
    for s in range(seqs):
        for h in range(heads):
            com_ref[s, h] = cm_l[s, :, h * size : (h + 1) * size]

    at, of = iota((per * seqs, per * seqs), 0), iota((per * seqs, per * seqs), 1)
    weave = jnp.zeros((per * seqs, per * seqs), F32)
    for s in range(seqs):
        weave = jnp.where(at == (of - s * per) * seqs + s, jnp.where((of >= s * per) & (of < (s + 1) * per), 1.0, weave), weave)
    weave = weave.astype(BF16)
    for ch in range(chunks):
        both = jnp.concatenate([final(s, ch, narrow[s].get(plan[s][ch])) for s in range(seqs)], axis=0)
        both = dot(weave, both.astype(BF16)).astype(BF16)
        for d in range(per):
            out_ref[d, :, piece_of(ch)] = both[d * seqs : (d + 1) * seqs]

    others = pl.ds(0, n_tok - 1)
    most = pl.ds(0, (n_tok - 1) * block)
    take(sent.at[0], q_l.at[:, most, :])
    take(sent.at[1], bc_l.at[:, :, most, :])
    take(sent.at[3], turn_v.at[:, :, pl.ds(0, (n_tok - 1) * width)])
    take(sent.at[4], xz_v.at[:, :, :, pl.ds(0, (n_tok - 1) * width)])
    take(sent.at[5], n_s.at[others])
    take(sent.at[6], stat_l.at[others])
    take(sent.at[7], ss_l.at[:, pl.ds(0, group - 1)])
    take(sent.at[8], pair_l)
    take(sent.at[9], cm_s.at[:, pl.ds(0, (n_tok - 1) * cols), :])
    for k, share_of in enumerate(sorted(set(counts))):
        same = pl.ds(counts.index(share_of), counts.count(share_of))
        a, b = pl.ds(0, share_of * span), pl.ds(0, (chunks - share_of) * span)
        if share_of:
            take(sent.at[10 + 4 * k], one_a.at[same, pl.ds(1, lines - 1), :, :, a])
            take(sent.at[12 + 4 * k], two_a.at[same, pl.ds(1, n_head - 1), :, a])
        if share_of < chunks:
            take(sent.at[11 + 4 * k], one_b.at[same, pl.ds(1, n_head - 1), :, :, b])
            take(sent.at[13 + 4 * k], two_b.at[same, pl.ds(1, lines - 1), :, b])


def finish(out_v, ctx_v, com_v, out_ref, ctx_ref, com_ref, sems):
    copies = [
        pltpu.make_async_copy(src, dst, sems.at[i])
        for i, (src, dst) in enumerate(((out_v, out_ref), (com_v, com_ref), (ctx_v, ctx_ref)))
    ]
    for copy in copies:
        copy.start()
    for copy in copies:
        copy.wait()


def body(
    mamba_input, gate_input, in_b, in_c, step_size, decay_rate, skip_weight, norm_gain,
    ssm_state, out_weight, queries, draft_token_keys, draft_values, cached_key_rows,
    cache_values, cache_len, accepted,
):
    n_tok = lax.axis_size("tok")
    n_head = lax.axis_size("head")
    group = n_head * n_tok
    lines = n_tok // 2
    seqs, block, features = mamba_input.shape
    heads = decay_rate.shape[0]
    size = features // heads
    cols = ssm_state.shape[3]
    state = cols * n_tok
    draft = block * n_tok
    width = features // n_tok
    att = draft_token_keys.shape[2]
    per_kv = queries.shape[2] // att
    cache = cached_key_rows.shape[1]
    out_cols = out_weight.shape[1]
    per = draft // group
    plan = [PLAN[min(s, len(PLAN) - 1)] for s in range(seqs)]
    chunks = len(plan[0])
    hops = max(lines, n_head) - 1
    turned = jnp.transpose(ssm_state, (0, 1, 3, 2))
    shapes = (
        (per, seqs, out_cols),
        (seqs, block, per_kv * att),
        (seqs, heads, cols, size),
    )
    operands = (
        mamba_input, gate_input, in_b, in_c, step_size, turned, queries, cached_key_rows,
        cache_values, out_weight, draft_token_keys, draft_values,
        norm_gain.reshape(1, features), decay_rate, skip_weight, cache_len, accepted,
    )
    vmem = pl.BlockSpec(memory_space=pltpu.VMEM)
    held = pl.pallas_call(
        functools.partial(kernel, (n_head, n_tok, seqs, block, heads, plan)),
        out_shape=[pltpu.VMEM(shape, BF16) for shape in shapes],
        in_specs=[pl.BlockSpec(memory_space=pltpu.HBM)] * len(operands),
        out_specs=[vmem] * 3,
        scratch_shapes=[
            pltpu.VMEM((seqs, 2, block, features), BF16),
            pltpu.VMEM((seqs, 2, draft, width), BF16),
            pltpu.VMEM((3, seqs, draft, state), BF16),
            pltpu.VMEM((seqs, block, heads), BF16),
            pltpu.VMEM((seqs, heads, cols, size), BF16),
            pltpu.VMEM((seqs, cols, features), BF16),
            pltpu.VMEM((seqs, state, width), BF16),
            pltpu.VMEM((seqs, draft, per_kv * att), BF16),
            pltpu.VMEM((2, seqs, cache, att), BF16),
            pltpu.VMEM((2, seqs, block, att), BF16),
            pltpu.VMEM(out_weight.shape, BF16),
            pltpu.VMEM((1, features), F32),
            pltpu.VMEM((seqs, group, 1, draft), F32),
            pltpu.VMEM((seqs, state, width), BF16),
            pltpu.VMEM((seqs, cols, features), BF16),
            pltpu.VMEM((n_tok, seqs, per_kv * block, att), BF16),
            pltpu.VMEM((n_tok, seqs, per_kv * block, att), BF16),
            pltpu.VMEM((n_tok, seqs, 1, per_kv * block), F32),
            pltpu.VMEM((n_tok, seqs, 1, per_kv * block), F32),
            pltpu.VMEM((seqs, 2, n_head, lines, per, out_cols), BF16),
            pltpu.VMEM((seqs, n_head, lines, per, out_cols), BF16),
            pltpu.VMEM((seqs, n_head, lines, per, out_cols), BF16),
            pltpu.VMEM((seqs, lines, n_head, per, out_cols), BF16),
            pltpu.VMEM((seqs, n_head, lines, per, out_cols), BF16),
            pltpu.VMEM((seqs, n_head, per, out_cols), BF16),
            pltpu.VMEM((seqs, lines, per, out_cols), BF16),
            pltpu.VMEM((seqs, n_head, per, out_cols), BF16),
            pltpu.VMEM((seqs, lines, per, out_cols), BF16),
            pltpu.SMEM((2,) + decay_rate.shape, F32),
            pltpu.SMEM((2,) + cache_len.shape, jnp.int32),
            pltpu.SemaphoreType.DMA((10 + 4 * len({row.count("A") for row in plan}),)),
            pltpu.SemaphoreType.DMA((n_tok - 1,)),
            pltpu.SemaphoreType.DMA((lines,)),
            pltpu.SemaphoreType.DMA((seqs,)),
            pltpu.SemaphoreType.DMA((seqs,)),
            pltpu.SemaphoreType.DMA((3,)),
            pltpu.SemaphoreType.DMA((seqs,)),
            pltpu.SemaphoreType.DMA((seqs, chunks)),
            pltpu.SemaphoreType.DMA((seqs, chunks, hops)),
            pltpu.SemaphoreType.DMA((seqs, chunks, hops)),
            pltpu.SemaphoreType.DMA((11,)),
        ],
        compiler_params=pltpu.CompilerParams(
            collective_id=0, has_side_effects=True, vmem_limit_bytes=40 * 1024 * 1024
        ),
        name="hybrid",
    )(*[pltpu.with_memory_space_constraint(a, pltpu.HBM) for a in operands])
    out, ctx, com = pl.pallas_call(
        finish,
        out_shape=[jax.ShapeDtypeStruct(shape, BF16) for shape in shapes],
        in_specs=[vmem] * 3,
        out_specs=[pl.BlockSpec(memory_space=pl.ANY)] * 3,
        scratch_shapes=[pltpu.SemaphoreType.DMA((3,))],
        compiler_params=pltpu.CompilerParams(vmem_limit_bytes=4 * 1024 * 1024),
        name="finish",
    )(*[pltpu.with_memory_space_constraint(a, pltpu.VMEM) for a in held])
    return (out, ctx, jnp.transpose(com, (0, 1, 3, 2)))


def solution(mesh):
    in_specs = (
        P("dp", "tok", "head"),
        P("dp", "tok", "head"),
        P("dp", "tok", "head"),
        P("dp", "tok", "head"),
        P("dp", "tok", "head"),
        P("head"),
        P("head"),
        P("head"),
        P("dp", "head", None, "tok"),
        P(("head", "tok"), None),
        P("dp", "tok", "head"),
        P("dp", "tok", "head"),
        P("dp", "tok", "head"),
        P("dp", "tok", "head"),
        P("dp", "tok", "head"),
        P("dp"),
        P("dp"),
    )
    out_specs = (
        P(("head", "tok"), "dp", None),
        P("dp", "tok", "head"),
        P("dp", "head", None, "tok"),
    )
    return jax.shard_map(body, mesh=mesh, in_specs=in_specs, out_specs=out_specs, check_vma=False)
```

```python
import functools
import jax
import jax.numpy as jnp
from jax import lax
from jax.experimental import pallas as pl
from jax.experimental.pallas import tpu as pltpu
from jax.sharding import PartitionSpec as P

EPSILON = 1e-05
MASKED = -1e30
FLOOR = -1e29
MESH = pl.DeviceIdType.MESH
F32 = jnp.float32
BF16 = jnp.bfloat16
NT = (((1,), (1,)), ((), ()))


def dot(a, b):
    return jnp.dot(a, b, preferred_element_type=F32)


def iota(shape, dim):
    return lax.broadcasted_iota(jnp.int32, shape, dim)


PLAN = ("ABAB", "ABAB")
EARLY = (0,)
LATE = 0
WEAVE = 2
FIRST = 0
POWER = False
LOG2E = 1.4426950408889634


def kernel(
    dims,
    x_in, z_in, b_in, c_in, dt_in, st_in, q_in, k_in, v_in, w_in,
    dk_in, dv_in, gain_in, rate_in, skip_in, len_in, acc_in,
    out_ref, ctx_ref, com_ref,
    xz_v, xz_l, bc_l, dt_v, raw_v, turn_v, st_l, q_l, kv_v, new_v, w_v, gain_v,
    ss_l, cm_s, cm_l, n_s, n_l, stat_s, stat_l,
    part, pair_l, red, one_a, one_b, mid_a, mid_b, two_a, two_b,
    heads_ref, seqs_ref,
    sent, q_recv, bc_recv, st_recv, xz_recv, got, ss_recv,
    pair_recv, one_recv, two_recv, local,
):
    n_head, n_tok, seqs, block, heads, plan = dims
    chunks = len(plan[0])
    counts = [row.count("A") for row in plan]
    kinds = [sorted(set(counts)).index(count) for count in counts]
    group = n_head * n_tok
    tok = lax.axis_index("tok")
    head = lax.axis_index("head")
    me = head * n_tok + tok
    draft = block * n_tok
    width = xz_l.shape[3]
    own = heads // n_tok
    size = width // own
    state = st_l.shape[1]
    cols = state // n_tok
    att = kv_v.shape[3]
    per_kv = q_l.shape[2] // att
    cache = kv_v.shape[2]
    per = draft // group
    out_cols = w_v.shape[1]
    span = out_cols // chunks
    half = group // 2
    side = lax.rem(tok, 2)
    line = tok // 2
    lines = n_tok // 2
    slot = head * lines + line

    def place(index, unit):
        return pl.ds(pl.multiple_of(index * unit, unit), unit)

    barrier = pltpu.get_barrier_semaphore()
    for o in range(1, group):
        peer = lax.rem(me + o, group)
        pl.semaphore_signal(
            barrier, inc=1,
            device_id={"head": peer // n_tok, "tok": lax.rem(peer, n_tok)},
            device_id_type=MESH,
        )

    def take(sem, ref):
        pltpu.make_async_copy(ref, ref, sem).wait()

    mine = place(tok, block)
    for sem, src, dst in (
        (0, st_in, raw_v),
        (1, q_in, q_l.at[:, mine, :]),
        (2, b_in, bc_l.at[0, :, mine, :]),
        (2, c_in, bc_l.at[1, :, mine, :]),
        (3, dt_in, dt_v),
        (4, x_in, xz_v.at[:, 0]),
        (4, z_in, xz_v.at[:, 1]),
        (5, dk_in, new_v.at[0]),
        (5, dv_in, new_v.at[1]),
        (6, k_in, kv_v.at[0]),
        (6, v_in, kv_v.at[1]),
        (7, len_in, seqs_ref.at[0]),
        (7, acc_in, seqs_ref.at[1]),
        (8, rate_in, heads_ref.at[0]),
        (8, skip_in, heads_ref.at[1]),
        (9, gain_in, gain_v),
        (10, w_in, w_v),
    ):
        pltpu.make_async_copy(src, dst, local.at[sem]).start()

    take(local.at[0], raw_v)
    for s in range(seqs):
        turn_v[s] = jnp.concatenate(
            [raw_v[s, h].astype(F32) for h in range(heads)], axis=1
        ).astype(BF16)
    st_l[:, place(tok, cols), :] = turn_v[:, :, place(tok, width)]
    take(local.at[1], q_l.at[:, mine, :])
    take(local.at[2], bc_l.at[pl.ds(0, 2), :, mine, :])
    take(local.at[3], dt_v)
    pad = jnp.zeros((seqs, block, state - heads), BF16)
    bc_l[2, :, mine, :] = jnp.concatenate([dt_v[...], pad], axis=2)
    take(local.at[4], xz_v)
    xz_l[:, :, mine, :] = xz_v[:, :, :, place(tok, width)]

    pl.semaphore_wait(barrier, group - 1)

    def remote(kind, src, dst, recv_sem, device):
        pltpu.make_async_remote_copy(
            src_ref=src, dst_ref=dst, send_sem=sent.at[kind], recv_sem=recv_sem,
            device_id=device, device_id_type=MESH,
        ).start()

    flip = tok + 1 - 2 * side
    partner = {"tok": flip}

    def share(at, device, q_sem, sem, only=None):
        span_at = place(at, block)
        for kind, ref, recv in (
            (0, q_l.at[:, span_at, :], q_recv.at[q_sem]),
            (1, bc_l.at[:, :, span_at, :], bc_recv.at[sem]),
        ):
            if only is None or kind in only:
                remote(kind, ref, ref, recv, device)

    def across(o):
        return lax.rem(line + o, lines) * 2 + lax.rem(side + o, 2)

    def origin(o, near):
        return lax.rem(line - o + lines, lines) * 2 + lax.rem(near + o, 2)

    for o in range(1, lines):
        share(tok, {"tok": across(o)}, o, o)
    share(tok, partner, 0, 0)
    for s in range(seqs):
        for o in range(1, n_tok):
            to = lax.rem(tok + o, n_tok)
            remote(
                3, turn_v.at[s, :, place(to, width)], st_l.at[s, place(tok, cols), :],
                st_recv.at[s], {"tok": to},
            )
        for o in range(1, n_tok):
            to = lax.rem(tok + o, n_tok)
            remote(
                4, xz_v.at[s, :, :, place(to, width)], xz_l.at[s, :, mine, :],
                xz_recv.at[s], {"tok": to},
            )

    take(local.at[7], seqs_ref)
    take(local.at[8], heads_ref)
    take(local.at[5], new_v)
    take(local.at[6], kv_v)
    scale = att ** (-0.5)
    m_own = per_kv * block
    eye = iota((m_own, m_own), 0) == iota((m_own, m_own), 1)
    position = tok * cache + iota((1, cache), 1)

    def attend(at, count):
        first, height = at * count, count * block
        inner = iota((height, block), 1) - iota((height, block), 0)
        inner = jnp.concatenate([inner] * per_kv, axis=0)
        r, lanes = (iota((per_kv * height, m_own), d) for d in range(2))
        picks = []
        for c in range(count):
            pick = None
            for h in range(per_kv):
                t = r - (h * count + c) * block
                hit = (t >= 0) & (t < block) & (lanes == h * block + t)
                pick = hit if pick is None else pick | hit
            picks.append(pick)
        each = range(seqs)
        q = [
            jnp.concatenate(
                [q_l[s, place(at, height), h * att : (h + 1) * att] for h in range(per_kv)], axis=0
            )
            for s in each
        ]
        old = [lax.dot_general(q[s], kv_v[0, s], NT, preferred_element_type=F32) for s in each]
        new = [lax.dot_general(q[s], new_v[0, s], NT, preferred_element_type=F32) for s in each]
        old = [jnp.where(position < seqs_ref[0, s], old[s], MASKED) for s in each]
        new = [jnp.where(inner <= (first - tok) * block, new[s], MASKED) for s in each]
        peak = [
            jnp.maximum(
                jnp.max(old[s], axis=1, keepdims=True), jnp.max(new[s], axis=1, keepdims=True)
            )
            for s in each
        ]
        peak = [jnp.maximum(peak[s], FLOOR) for s in each]
        if POWER:
            lift = [peak[s] * (scale * LOG2E) for s in each]
            old = [jnp.exp2(old[s] * (scale * LOG2E) - lift[s]) for s in each]
            new = [jnp.exp2(new[s] * (scale * LOG2E) - lift[s]) for s in each]
        else:
            old = [jnp.exp((old[s] - peak[s]) * scale) for s in each]
            new = [jnp.exp((new[s] - peak[s]) * scale) for s in each]
        numer = [dot(old[s].astype(BF16), kv_v[1, s]) for s in each]
        numer = [numer[s] + dot(new[s].astype(BF16), new_v[1, s]) for s in each]
        total = [
            jnp.sum(old[s], axis=1, keepdims=True) + jnp.sum(new[s], axis=1, keepdims=True)
            for s in each
        ]
        for s in each:
            safe = jnp.maximum(total[s], 1e-30)
            level = jnp.where(total[s] > 0.0, peak[s] * scale + jnp.log(safe), MASKED)
            ctx = (numer[s] / safe).astype(BF16)
            for c in range(count):
                for h in range(per_kv):
                    n_s[first + c, s, h * block : (h + 1) * block] = ctx[
                        (h * count + c) * block : (h * count + c + 1) * block
                    ]
                stat_s[first + c, s] = jnp.sum(
                    jnp.where(picks[c], level, 0.0), axis=0, keepdims=True
                )

    def answer(t):
        remote(5, n_s.at[t], n_l.at[tok], got.at[0], {"tok": t})
        remote(6, stat_s.at[t], stat_l.at[tok], got.at[1], {"tok": t})

    take(q_recv.at[0], q_l.at[:, mine, :])
    attend(line, 2)
    answer(flip)
    n_l[tok] = n_s[tok]
    stat_l[tok] = stat_s[tok]
    for o in range(1, lines):
        take(q_recv.at[o], q_l.at[:, mine, :])
        share(origin(o, side), partner, lines - 1 + o, 0, (0,))
    for o in range(1, lines):
        attend(origin(o, side), 1)
        answer(origin(o, side))
    for o in range(1, lines):
        take(bc_recv.at[o], bc_l.at[:, :, mine, :])
        share(origin(o, side), partner, 0, 0, (1,))
    for o in range(1, lines):
        take(q_recv.at[lines - 1 + o], q_l.at[:, mine, :])
        attend(origin(o, 1 - side), 1)
        answer(origin(o, 1 - side))

    lane = iota((1, width), 1)
    rate_x = jnp.zeros((1, width), F32)
    skip_x = jnp.zeros((1, width), F32)
    for h in range(own):
        inside = (lane >= h * size) & (lane < (h + 1) * size)
        rate_x = jnp.where(inside, heads_ref[0, tok * own + h], rate_x)
        skip_x = jnp.where(inside, heads_ref[1, tok * own + h], skip_x)
    offset = iota((state, width), 1) - (iota((state, width), 0) - tok * own) * size
    pick = ((offset >= 0) & (offset < size)).astype(F32).astype(BF16)
    causal = iota((draft, draft), 0) >= iota((draft, draft), 1)
    lower = causal.astype(F32).astype(BF16)

    level_eye = iota((draft, draft), 0) == iota((draft, draft), 1)
    take(local.at[9], gain_v)
    gain = gain_v[:, place(tok, width)]
    take(local.at[10], w_v)
    take(bc_recv.at[0], bc_l.at[:, :, pl.ds(0, lines * block), :])
    early = {}

    def prepare(s):
        dtx = dot(bc_l[2, s], pick)
        run = -rate_x * dot(lower, dtx.astype(BF16))
        mix = lax.dot_general(bc_l[1, s], bc_l[0, s], NT, preferred_element_type=F32)
        mix = jnp.where(causal, mix, 0.0).astype(BF16)
        alive = iota((draft, width), 0) < seqs_ref[1, s]
        end = -rate_x * jnp.sum(jnp.where(alive, dtx, 0.0), axis=0, keepdims=True)
        weight = jnp.where(alive, jnp.exp(jnp.where(alive, end - run, 0.0)) * dtx, 0.0)
        flow = bc_l[0, s].astype(F32).T.astype(BF16)
        early[s] = (mix, jnp.exp(run), dtx * jnp.exp(-run), weight, jnp.exp(end), flow)

    prepare(0)

    tile = min(512, span)

    def piece_of(ch):
        return pl.ds(ch * span, span)

    def mix_tokens(s):
        x = xz_l[s, 0].astype(F32)
        z = xz_l[s, 1].astype(F32)
        mix, grown, shrunk = early[s][:3]
        inside = dot(mix, (x * shrunk).astype(BF16))
        y = grown * (inside + dot(bc_l[1, s], st_l[s])) + skip_x * x
        gated = y * z / (1.0 + jnp.exp(-z))
        return gated

    def spread(s, gated):
        sums = jnp.sum(gated * gated, axis=1, keepdims=True)
        ss_l[s, me] = jnp.sum(jnp.where(level_eye, sums, 0.0), axis=0, keepdims=True)
        for o in range(1, group):
            peer = lax.rem(me + o, group)
            remote(
                7, ss_l.at[s, me], ss_l.at[s, me], ss_recv.at[s],
                {"head": peer // n_tok, "tok": lax.rem(peer, n_tok)},
            )

    def project(s, normed, between):
        for ch in range(chunks):
            for start in range(ch * span, (ch + 1) * span, tile):
                val = dot(normed, w_v[:, start : start + tile])
                for g in range(half):
                    for p in range(2):
                        at = (g * 2 + p) * per
                        hold = lax.rem(p + head + line + g // lines + g % lines, 2)
                        part[s, hold, g // lines, g % lines, :, start : start + tile] = val[
                            at : at + per
                        ].astype(BF16)
            remote(
                8, part.at[s, 1 - side, :, :, :, piece_of(ch)],
                pair_l.at[s, :, :, :, piece_of(ch)], pair_recv.at[s, ch], partner,
            )
            between(ch)

    def commit(s):
        x = xz_l[s, 0].astype(F32)
        weight, decay, flow = early[s][3:]
        new = decay * st_l[s].astype(F32) + dot(flow, (x * weight).astype(BF16))
        cm_s[s] = new.astype(BF16)
        cm_l[s, :, place(tok, width)] = cm_s[s, place(tok, cols), :]

    def hand_out(s):
        for o in range(1, n_tok):
            to = lax.rem(tok + o, n_tok)
            remote(
                9, cm_s.at[s, place(to, cols), :], cm_l.at[s, :, place(tok, width)],
                got.at[2], {"tok": to},
            )

    def above(o):
        return {"head": lax.rem(head + o, n_head), "tok": line * 2 + lax.rem(side + o, 2)}

    def forward(s, ch):
        piece = piece_of(ch)
        take(pair_recv.at[s, ch], pair_l.at[s, :, :, :, piece])
        red[s, :, :, :, piece] = (
            part[s, side, :, :, :, piece].astype(F32) + pair_l[s, :, :, :, piece].astype(F32)
        ).astype(BF16)
        if plan[s][ch] == "A":
            for o in range(1, lines):
                to = lax.rem(line + o, lines)
                remote(
                    10 + 4 * kinds[s], red.at[s, :, to, :, piece], one_a.at[s, o, :, :, piece],
                    one_recv.at[s, ch, o - 1], {"tok": across(o)},
                )
        else:
            for o in range(1, n_head):
                to = lax.rem(head + o, n_head)
                remote(
                    11 + 4 * kinds[s], red.at[s, to, :, :, piece], one_b.at[s, o, :, :, piece],
                    one_recv.at[s, ch, o - 1], above(o),
                )

    def factor(s, source, base):
        total = jnp.zeros((1, draft), F32)
        for t in range(n_tok):
            total = total + ss_l[s, source * n_tok + t]
        here = iota((per, draft), 1) == base * per + iota((per, draft), 0)
        column = jnp.sum(jnp.where(here, total, 0.0), axis=1, keepdims=True)
        return lax.rsqrt(column / (width * n_tok) + EPSILON)

    def second(s, ch, factors):
        piece = piece_of(ch)
        if plan[s][ch] == "A":
            for o in range(1, lines):
                take(one_recv.at[s, ch, o - 1], one_a.at[s, o, :, :, piece])
            total = red[s, :, line, :, piece].astype(F32)
            for o in range(1, lines):
                total = total + one_a[s, o, :, :, piece].astype(F32)
            mid_a[s, :, :, piece] = total.astype(BF16)
            for o in range(1, n_head):
                to = lax.rem(head + o, n_head)
                remote(
                    12 + 4 * kinds[s], mid_a.at[s, to, :, piece], two_a.at[s, o, :, piece],
                    two_recv.at[s, 0, o - 1], above(o),
                )
        else:
            for o in range(1, n_head):
                take(one_recv.at[s, ch, o - 1], one_b.at[s, o, :, :, piece])
            for l in range(lines):
                total = red[s, head, l, :, piece].astype(F32) * factors[0][l]
                for o in range(1, n_head):
                    total = total + one_b[s, o, l, :, piece].astype(F32) * factors[o][l]
                mid_b[s, l, :, piece] = total.astype(BF16)
            for o in range(1, lines):
                to = lax.rem(line + o, lines)
                remote(
                    13 + 4 * kinds[s], mid_b.at[s, to, :, piece], two_b.at[s, o, :, piece],
                    two_recv.at[s, 1, o - 1], {"tok": across(o)},
                )

    def final(s, ch, factors):
        piece = piece_of(ch)
        if plan[s][ch] == "A":
            total = mid_a[s, head, :, piece].astype(F32) * factors[0]
            for o in range(1, n_head):
                total = total + two_a[s, o, :, piece].astype(F32) * factors[o]
        else:
            total = mid_b[s, line, :, piece].astype(F32)
            for o in range(1, lines):
                total = total + two_b[s, o, :, piece].astype(F32)
        return total

    for s in range(seqs):
        take(st_recv.at[s], st_l.at[s, pl.ds(0, (n_tok - 1) * cols), :])
        take(xz_recv.at[s], xz_l.at[s, :, pl.ds(0, (n_tok - 1) * block), :])
        if FIRST == 0 and s in EARLY:
            commit(s)
            hand_out(s)
        gated = mix_tokens(s)

        def between(ch, s=s):
            if s > 0 and ch + WEAVE < chunks:
                forward(s - 1, ch + WEAVE)

        project(s, (gated * gain).astype(BF16), between)
        spread(s, gated)
        if s not in EARLY or FIRST > 0:
            commit(s)
            if s in EARLY and FIRST == 1:
                hand_out(s)
        if s + 1 < seqs:
            prepare(s + 1)
        for ch in range(chunks if s == seqs - 1 else min(WEAVE, chunks)):
            forward(s, ch)
        if FIRST == 3 and s in EARLY:
            hand_out(s)
    for s in range(seqs):
        if FIRST == 2 and s in EARLY:
            hand_out(s)

    narrow = []
    for s in range(seqs):
        take(ss_recv.at[s], ss_l.at[s, pl.ds(0, group - 1)])
        sources = [lax.rem(head - o + n_head, n_head) for o in range(n_head)]
        places = [(head * lines + l) * 2 + lax.rem(side + line + l, 2) for l in range(lines)]
        wide = None
        if "B" in plan[s]:
            wide = [[factor(s, source, at) for at in places] for source in sources]
        near = {}
        if "A" in plan[s]:
            near["A"] = [factor(s, source, me) for source in sources]
        narrow.append(near)
        for ch in range(chunks):
            second(s, ch, wide)
        if s == LATE:
            for later in range(seqs):
                if later not in EARLY:
                    hand_out(later)

    take(got.at[0], n_l.at[pl.ds(0, n_tok - 1)])
    take(got.at[1], stat_l.at[pl.ds(0, n_tok - 1)])
    for s in range(seqs):
        levels = [
            jnp.sum(jnp.where(eye, stat_l[t, s], 0.0), axis=1, keepdims=True)
            for t in range(n_tok)
        ]
        top = functools.reduce(jnp.maximum, levels)
        weights = [jnp.exp(level - top) for level in levels]
        den = functools.reduce(jnp.add, weights)
        acc = jnp.zeros((m_own, att), F32)
        for t in range(n_tok):
            acc = acc + weights[t] * n_l[t, s].astype(F32)
        acc = (acc / den).astype(BF16)
        for h in range(per_kv):
            ctx_ref[s, :, h * att : (h + 1) * att] = acc[h * block : (h + 1) * block]

    take(got.at[2], cm_l.at[:, :, pl.ds(0, (n_tok - 1) * width)])
    for s in range(seqs):
        for h in range(heads):
            com_ref[s, h] = cm_l[s, :, h * size : (h + 1) * size]

    at, of = iota((per * seqs, per * seqs), 0), iota((per * seqs, per * seqs), 1)
    weave = jnp.zeros((per * seqs, per * seqs), F32)
    for s in range(seqs):
        weave = jnp.where(at == (of - s * per) * seqs + s, jnp.where((of >= s * per) & (of < (s + 1) * per), 1.0, weave), weave)
    weave = weave.astype(BF16)
    for s in range(seqs):
        a, b = pl.ds(0, counts[s] * span), pl.ds(0, (chunks - counts[s]) * span)
        if counts[s]:
            for o in range(1, n_head):
                take(two_recv.at[s, 0, o - 1], two_a.at[s, o, :, a])
        if counts[s] < chunks:
            for o in range(1, lines):
                take(two_recv.at[s, 1, o - 1], two_b.at[s, o, :, b])
    for ch in range(chunks):
        both = jnp.concatenate([final(s, ch, narrow[s].get(plan[s][ch])) for s in range(seqs)], axis=0)
        both = dot(weave, both.astype(BF16)).astype(BF16)
        for d in range(per):
            out_ref[d, :, piece_of(ch)] = both[d * seqs : (d + 1) * seqs]

    others = pl.ds(0, n_tok - 1)
    most = pl.ds(0, (n_tok - 1) * block)
    take(sent.at[0], q_l.at[:, most, :])
    take(sent.at[1], bc_l.at[:, :, most, :])
    take(sent.at[3], turn_v.at[:, :, pl.ds(0, (n_tok - 1) * width)])
    take(sent.at[4], xz_v.at[:, :, :, pl.ds(0, (n_tok - 1) * width)])
    take(sent.at[5], n_s.at[others])
    take(sent.at[6], stat_l.at[others])
    take(sent.at[7], ss_l.at[:, pl.ds(0, group - 1)])
    take(sent.at[8], pair_l)
    take(sent.at[9], cm_s.at[:, pl.ds(0, (n_tok - 1) * cols), :])
    for k, share_of in enumerate(sorted(set(counts))):
        same = pl.ds(counts.index(share_of), counts.count(share_of))
        a, b = pl.ds(0, share_of * span), pl.ds(0, (chunks - share_of) * span)
        if share_of:
            take(sent.at[10 + 4 * k], one_a.at[same, pl.ds(1, lines - 1), :, :, a])
            take(sent.at[12 + 4 * k], two_a.at[same, pl.ds(1, n_head - 1), :, a])
        if share_of < chunks:
            take(sent.at[11 + 4 * k], one_b.at[same, pl.ds(1, n_head - 1), :, :, b])
            take(sent.at[13 + 4 * k], two_b.at[same, pl.ds(1, lines - 1), :, b])


def finish(out_v, ctx_v, com_v, out_ref, ctx_ref, com_ref, sems):
    copies = [
        pltpu.make_async_copy(src, dst, sems.at[i])
        for i, (src, dst) in enumerate(((out_v, out_ref), (com_v, com_ref), (ctx_v, ctx_ref)))
    ]
    for copy in copies:
        copy.start()
    for copy in copies:
        copy.wait()


def body(
    mamba_input, gate_input, in_b, in_c, step_size, decay_rate, skip_weight, norm_gain,
    ssm_state, out_weight, queries, draft_token_keys, draft_values, cached_key_rows,
    cache_values, cache_len, accepted,
):
    n_tok = lax.axis_size("tok")
    n_head = lax.axis_size("head")
    group = n_head * n_tok
    lines = n_tok // 2
    seqs, block, features = mamba_input.shape
    heads = decay_rate.shape[0]
    size = features // heads
    cols = ssm_state.shape[3]
    state = cols * n_tok
    draft = block * n_tok
    width = features // n_tok
    att = draft_token_keys.shape[2]
    per_kv = queries.shape[2] // att
    cache = cached_key_rows.shape[1]
    out_cols = out_weight.shape[1]
    per = draft // group
    plan = [PLAN[min(s, len(PLAN) - 1)] for s in range(seqs)]
    chunks = len(plan[0])
    hops = max(lines, n_head) - 1
    turned = jnp.transpose(ssm_state, (0, 1, 3, 2))
    shapes = (
        (per, seqs, out_cols),
        (seqs, block, per_kv * att),
        (seqs, heads, cols, size),
    )
    operands = (
        mamba_input, gate_input, in_b, in_c, step_size, turned, queries, cached_key_rows,
        cache_values, out_weight, draft_token_keys, draft_values,
        norm_gain.reshape(1, features), decay_rate, skip_weight, cache_len, accepted,
    )
    vmem = pl.BlockSpec(memory_space=pltpu.VMEM)
    held = pl.pallas_call(
        functools.partial(kernel, (n_head, n_tok, seqs, block, heads, plan)),
        out_shape=[pltpu.VMEM(shape, BF16) for shape in shapes],
        in_specs=[pl.BlockSpec(memory_space=pltpu.HBM)] * len(operands),
        out_specs=[vmem] * 3,
        scratch_shapes=[
            pltpu.VMEM((seqs, 2, block, features), BF16),
            pltpu.VMEM((seqs, 2, draft, width), BF16),
            pltpu.VMEM((3, seqs, draft, state), BF16),
            pltpu.VMEM((seqs, block, heads), BF16),
            pltpu.VMEM((seqs, heads, cols, size), BF16),
            pltpu.VMEM((seqs, cols, features), BF16),
            pltpu.VMEM((seqs, state, width), BF16),
            pltpu.VMEM((seqs, draft, per_kv * att), BF16),
            pltpu.VMEM((2, seqs, cache, att), BF16),
            pltpu.VMEM((2, seqs, block, att), BF16),
            pltpu.VMEM(out_weight.shape, BF16),
            pltpu.VMEM((1, features), F32),
            pltpu.VMEM((seqs, group, 1, draft), F32),
            pltpu.VMEM((seqs, state, width), BF16),
            pltpu.VMEM((seqs, cols, features), BF16),
            pltpu.VMEM((n_tok, seqs, per_kv * block, att), BF16),
            pltpu.VMEM((n_tok, seqs, per_kv * block, att), BF16),
            pltpu.VMEM((n_tok, seqs, 1, per_kv * block), F32),
            pltpu.VMEM((n_tok, seqs, 1, per_kv * block), F32),
            pltpu.VMEM((seqs, 2, n_head, lines, per, out_cols), BF16),
            pltpu.VMEM((seqs, n_head, lines, per, out_cols), BF16),
            pltpu.VMEM((seqs, n_head, lines, per, out_cols), BF16),
            pltpu.VMEM((seqs, lines, n_head, per, out_cols), BF16),
            pltpu.VMEM((seqs, n_head, lines, per, out_cols), BF16),
            pltpu.VMEM((seqs, n_head, per, out_cols), BF16),
            pltpu.VMEM((seqs, lines, per, out_cols), BF16),
            pltpu.VMEM((seqs, n_head, per, out_cols), BF16),
            pltpu.VMEM((seqs, lines, per, out_cols), BF16),
            pltpu.SMEM((2,) + decay_rate.shape, F32),
            pltpu.SMEM((2,) + cache_len.shape, jnp.int32),
            pltpu.SemaphoreType.DMA((10 + 4 * len({row.count("A") for row in plan}),)),
            pltpu.SemaphoreType.DMA((n_tok - 1,)),
            pltpu.SemaphoreType.DMA((lines,)),
            pltpu.SemaphoreType.DMA((seqs,)),
            pltpu.SemaphoreType.DMA((seqs,)),
            pltpu.SemaphoreType.DMA((3,)),
            pltpu.SemaphoreType.DMA((seqs,)),
            pltpu.SemaphoreType.DMA((seqs, chunks)),
            pltpu.SemaphoreType.DMA((seqs, chunks, hops)),
            pltpu.SemaphoreType.DMA((seqs, 2, hops)),
            pltpu.SemaphoreType.DMA((11,)),
        ],
        compiler_params=pltpu.CompilerParams(
            collective_id=0, has_side_effects=True, vmem_limit_bytes=40 * 1024 * 1024
        ),
        name="hybrid",
    )(*[pltpu.with_memory_space_constraint(a, pltpu.HBM) for a in operands])
    out, ctx, com = pl.pallas_call(
        finish,
        out_shape=[jax.ShapeDtypeStruct(shape, BF16) for shape in shapes],
        in_specs=[vmem] * 3,
        out_specs=[pl.BlockSpec(memory_space=pl.ANY)] * 3,
        scratch_shapes=[pltpu.SemaphoreType.DMA((3,))],
        compiler_params=pltpu.CompilerParams(vmem_limit_bytes=4 * 1024 * 1024),
        name="finish",
    )(*[pltpu.with_memory_space_constraint(a, pltpu.VMEM) for a in held])
    return (out, ctx, jnp.transpose(com, (0, 1, 3, 2)))


def solution(mesh):
    in_specs = (
        P("dp", "tok", "head"),
        P("dp", "tok", "head"),
        P("dp", "tok", "head"),
        P("dp", "tok", "head"),
        P("dp", "tok", "head"),
        P("head"),
        P("head"),
        P("head"),
        P("dp", "head", None, "tok"),
        P(("head", "tok"), None),
        P("dp", "tok", "head"),
        P("dp", "tok", "head"),
        P("dp", "tok", "head"),
        P("dp", "tok", "head"),
        P("dp", "tok", "head"),
        P("dp"),
        P("dp"),
    )
    out_specs = (
        P(("head", "tok"), "dp", None),
        P("dp", "tok", "head"),
        P("dp", "head", None, "tok"),
    )
    return jax.shard_map(body, mesh=mesh, in_specs=in_specs, out_specs=out_specs, check_vma=False)
```
